256 devices in a mesh: dp: 32 (over z, y), tp: 8 (over x, core).
Axes of the slice: x: 4, y: 4, z: 8, core: 2. Of those that a mesh axis runs over, the one named last changes fastest.
Arguments:
- tokens: bfloat16 [3072, 2880], P('dp', 'tp'), may hold values from -100 to 100
- attn_gain: float32 [2880], replicated, may hold values from 0.1 to 1.9
- w_query: bfloat16 [2880, 2048], P(None, 'tp'), may hold values from -0.109375 to 0.109375
- w_keyvalue: bfloat16 [2880, 8, 128], P(None, 'tp'), may hold values from -0.109375 to 0.109375
- attn_sinks: float32 [32], P('tp'), may hold values from 2 to 6
- w_out: bfloat16 [2048, 2880], P('tp'), may hold values from -0.125 to 0.125
- window_cache: bfloat16 [3072, 8, 128, 128], P('dp', 'tp'), may hold values from -1000 to 1000
- positions: int32 [3072], P('dp'), may hold values from 0 to 511
- moe_gain: float32 [2880], replicated, may hold values from 0.1 to 1.9
- router: bfloat16 [2880, 32], P('tp'), may hold values from -0.109375 to 0.109375
- gate_up: bfloat16 [32, 2880, 2, 2880], P('dp', None, None, 'tp'), may hold values from -0.109375 to 0.109375
- w_down: bfloat16 [32, 2880, 2880], P('dp', None, 'tp'), may hold values from -0.109375 to 0.109375
- expert_ids: int32 [3072, 4], P('dp'), may hold values from 0 to 31, all different within a row; in each aligned block of 96 rows (0 to 95, 96 to 191, ...) at most 32 rows name the same one
Outputs:
- layer_out: float32 [3072, 2880], P('dp', 'tp')
The draws below stay inside these ranges and needn't reach their ends.
Inputs may be any that keep to these rules, and one draw needn't show every extreme that they name: `expert_ids`: each row names 4 different experts. Within the rows of one index of dp no expert is named by more than 32 rows, a bound that some of these blocks reach.
All inputs are finite; a program needn't handle non-finite values.
Results may differ from the reference program's by a relative error of at most 0.0066.
Values may be sent and summed in bfloat16 or wider, within the bound.
A program may use at most 128 MiB of HBM per device.

```python
import math
import jax
import jax.numpy as jnp
import numpy as np
from jax import lax

D = 2880
QH = 32
KVH = 8
HD = 64
WINDOW = 128
TOP = 4
FF = 2880
TOK_DEV = 96
EXPERTS = 32
TOKENS = 3072
CAP = 32
N_DP = 32


def draw_tokens(key, part):
    base_key, col_key, row_key = jax.random.split(key, 3)
    places = jnp.arange(D, dtype=jnp.float32) / D
    col_scale = jnp.power(10.0, 0.5 * places + 0.5 * jax.random.uniform(col_key, (D,)))
    base = jnp.clip(jax.random.normal(base_key, (TOKENS, D)), -4.0, 4.0)
    row_scale = jnp.power(10.0, jax.random.uniform(row_key, (TOKENS, 1)))
    return (0.1 * base * row_scale * col_scale[None, :]).astype(jnp.bfloat16)


def draw_window_cache(key, part):
    normal_key = jax.random.fold_in(key, 0)
    entries = jnp.clip(jax.random.normal(normal_key, (TOKENS, KVH, WINDOW, 2 * HD)), -6.0, 6.0)
    return entries.astype(jnp.bfloat16)


def touch_ends(result, key, smallest, high):
    spot = [jax.random.randint(jax.random.fold_in(key, axis), (), 0, length) for axis, length in enumerate(result.shape)]
    main_axis = result.shape.index(max(result.shape))
    next_to = spot[:main_axis] + [(spot[main_axis] + 1) % result.shape[main_axis]] + spot[main_axis + 1:]
    return result.at[tuple(spot)].set(smallest).at[tuple(next_to)].set(high)


def block_levels(key, extent, shards, smallest, high):
    loudness, own = 1.0, jax.random.fold_in(key, 6)
    for dim, parts in shards:
        draws = jnp.exp(jax.random.uniform(jax.random.fold_in(own, dim), (parts,), jnp.float32, smallest / len(shards), high / len(shards)))
        loudness = loudness * jnp.repeat(draws, extent[dim] // parts).reshape([-1 if axis == dim else 1 for axis in range(len(extent))])
    return loudness


def routed_block(own_key, own, number, rows, number_of, top, reach, slope):
    ranking = jax.random.permutation(own_key, number_of)
    crowded, ordinary = load_shares(number_of, rows * top, reach, slope, True), load_shares(number_of, rows * top, reach, slope, False)
    places = jnp.arange(number_of)

    def named(sizes, turn):
        used = int((sizes > 0).sum())
        fixed = max(1, used // 4)
        moved = fixed + (places - fixed + turn * (used - fixed)) % max(1, number_of - fixed)
        return jnp.zeros((number_of,), jnp.int32).at[ranking[jnp.where(places < fixed, places, moved)]].set(jnp.asarray(sizes, jnp.int32))

    sizes = jnp.where(number % 4 == 0, named(crowded, number // 4), named(ordinary, number - number // 4 - 1))
    mixed = jax.random.permutation(jax.random.fold_in(own, 3), number_of)
    donor, sink = mixed[0:number_of // 2 * 2:2], mixed[1:number_of // 2 * 2:2]
    slack = jnp.minimum(sizes[donor] - 1, reach - sizes[sink]) // 2
    slack = jnp.where((donor == ranking[0]) | (sink == ranking[0]) | (sizes[sink] == 0), 0, jnp.maximum(slack, 0))
    moved = jax.random.randint(jax.random.fold_in(own, 4), (number_of // 2,), 0, 1 << 20) % (slack + 1)
    sizes = sizes.at[donor].add(-moved).at[sink].add(moved)
    items = jnp.searchsorted(jnp.cumsum(sizes), jnp.arange(rows * top), side="right").astype(jnp.int32)
    listing = items.reshape(top, rows).T
    listing = listing[jax.random.permutation(jax.random.fold_in(own, 1), rows)]
    turn = jax.random.randint(jax.random.fold_in(own, 2), (rows, 1), 0, top)
    return jnp.take_along_axis(listing, (jnp.arange(top)[None, :] + turn) % top, axis=1)


def load_shares(number_of, total, limit, lean, full):
    weights = [(1 << 20) // math.isqrt(rank ** lean) + 1 for rank in range(1, number_of + 1)]
    largest = limit if full else min(limit, max(-(-total // number_of), total * weights[0] // sum(weights)))
    least = 1 if total - largest >= number_of - 1 else 0
    counts, surplus = [largest] + [least] * (number_of - 1), total - largest - least * (number_of - 1)
    while surplus > 0:
        candidates = [i for i in range(1, number_of) if counts[i] < largest] or [i for i in range(1, number_of) if counts[i] < limit]
        mass, left = sum([weights[i] for i in candidates]), surplus
        for i in candidates:
            more = min(limit - counts[i], max(1, left * weights[i] // mass), surplus)
            counts[i] = counts[i] + more
            surplus = surplus - more
    return np.array(counts)


def gaussian(stream_key, shape, spread, most, cuts=(), kind=jnp.bfloat16):
    drawn = spread * jax.random.normal(stream_key, shape, jnp.float32)
    if cuts:
        drawn = drawn * block_levels(stream_key, shape, cuts, -0.22, 0.18)
    return jnp.clip(drawn, -most, most).astype(kind)


def setup_inputs(seed: int = 0) -> dict:
    splits = jax.random.split(jax.random.key(seed), 14)
    tokens = draw_tokens(jax.random.fold_in(splits[13], 71), 0)
    attn_gain = jnp.clip(1.0 + 0.18 * jax.random.normal(splits[1], (D,), jnp.float32), 0.1, 1.9)
    w_query = gaussian(splits[2], (D, QH * HD), D ** -0.5, 0.109375, ((1, 8),))
    w_keyvalue = gaussian(splits[3], (D, KVH, 2 * HD), D ** -0.5, 0.109375, ((1, 8),))
    attn_sinks = jnp.clip(2.0 + 4.0 * jax.random.uniform(splits[4], (QH,), jnp.float32) ** block_levels(splits[4], (QH,), ((0, 8),), -0.2, 0.2), 2.0, 6.0)
    w_out = gaussian(splits[5], (QH * HD, D), (QH * HD) ** -0.5, 0.125, ((0, 8),))
    window_cache = draw_window_cache(jax.random.fold_in(splits[13], 71), 0)
    positions = touch_ends(jax.random.randint(splits[7], (TOKENS,), 0, 4 * WINDOW), jax.random.fold_in(splits[7], 1), 0, (4 * WINDOW) - 1).astype(jnp.int32)
    moe_gain = jnp.clip(1.0 + 0.18 * jax.random.normal(splits[8], (D,), jnp.float32), 0.1, 1.9)
    router = gaussian(splits[9], (D, EXPERTS), D ** -0.5, 0.109375, ((0, 8),))
    gate_up = gaussian(splits[10], (EXPERTS, D, 2, FF), D ** -0.5, 0.109375, ((0, 32), (3, 8)))
    w_down = gaussian(splits[11], (EXPERTS, FF, D), FF ** -0.5, 0.109375, ((0, 32), (2, 8)))
    expert_ids_keys = jax.random.split(jax.random.fold_in(splits[12], 1), TOKENS // TOK_DEV)
    expert_ids_turns = jax.random.permutation(jax.random.fold_in(splits[12], 3), TOKENS // TOK_DEV)
    expert_ids = jax.vmap(lambda own, number: routed_block(jax.random.fold_in(splits[12], 2), own, number, TOK_DEV, EXPERTS, TOP, CAP, 2))(expert_ids_keys, expert_ids_turns).reshape((TOKENS, TOP))
    return {"tokens": tokens, "attn_gain": attn_gain, "w_query": w_query, "w_keyvalue": w_keyvalue, "attn_sinks": attn_sinks, "w_out": w_out, "window_cache": window_cache, "positions": positions, "moe_gain": moe_gain, "router": router, "gate_up": gate_up, "w_down": w_down, "expert_ids": expert_ids}


norm_eps = 1e-05
rope_base = 150000.0
glu_alpha = 1.702

def rope_tables(positions, head_size):
    half_size = head_size // 2
    exponent = jnp.arange(half_size, dtype=jnp.float32) * (2.0 / head_size)
    inverse = jnp.power(jnp.float32(rope_base), -exponent)
    angles = positions.astype(jnp.float32)[:, None] * inverse[None, :]
    return (jnp.cos(angles), jnp.sin(angles))

def rotate(values, cosine, sine_table):
    half_size = values.shape[-1] // 2
    first_half = values[..., :half_size]
    second_half = values[..., half_size:]
    return jnp.concatenate([first_half * cosine - second_half * sine_table, second_half * cosine + first_half * sine_table], axis=-1)

def reference(tokens, attn_gain, w_query, w_keyvalue, attn_sinks, w_out, window_cache, positions, moe_gain, router, gate_up, w_down, expert_ids):
    seq_count, full_width = tokens.shape
    head_size = w_keyvalue.shape[2] // 2
    kv_heads = w_keyvalue.shape[1]
    q_heads = w_query.shape[1] // head_size
    group_size = q_heads // kv_heads
    window = window_cache.shape[2]
    tok_wide = tokens.astype(jnp.float32)
    attn_mean = lax.optimization_barrier(jnp.mean(tok_wide * tok_wide, axis=1, keepdims=True))
    normed = (tok_wide * lax.rsqrt(attn_mean + norm_eps) * attn_gain[None, :]).astype(jnp.bfloat16)
    queries = jnp.dot(normed, w_query, preferred_element_type=jnp.float32).reshape(seq_count, q_heads, head_size)
    fresh_rows = jnp.dot(normed, w_keyvalue.reshape(full_width, kv_heads * 2 * head_size), preferred_element_type=jnp.float32)
    fresh_rows = fresh_rows.reshape(seq_count, kv_heads, 2 * head_size)
    cosine, sine_table = rope_tables(positions, head_size)
    rot_queries = rotate(queries, cosine[:, None, :], sine_table[:, None, :]).astype(jnp.bfloat16)
    new_key = rotate(fresh_rows[..., :head_size], cosine[:, None, :], sine_table[:, None, :])
    new_entry = jnp.concatenate([new_key, fresh_rows[..., head_size:]], axis=-1).astype(jnp.bfloat16)
    slot_ids = jnp.arange(window, dtype=jnp.int32)
    is_current = slot_ids[None, :] == (positions % window)[:, None]
    cache_now = jnp.where(is_current[:, None, :, None], new_entry[:, :, None, :], window_cache)
    is_valid = (positions[:, None] - slot_ids[None, :]) % window <= positions[:, None]
    score_scale = head_size ** (-0.5)

    def attend_head(inputs):
        head_cache, head_query, head_sinks = inputs
        key_part = head_cache[..., :head_size].astype(jnp.float32)
        value_part = head_cache[..., head_size:].astype(jnp.float32)
        scores = jnp.einsum('sgh,swh->sgw', head_query.astype(jnp.float32), key_part) * score_scale
        scores = jnp.where(is_valid[:, None, :], scores, -jnp.inf)
        sink_col = head_sinks[None, :, None]
        peak_score = jnp.maximum(lax.optimization_barrier(jnp.max(scores, axis=-1, keepdims=True)), sink_col)
        raised = jnp.exp(scores - peak_score)
        denominator = lax.optimization_barrier(jnp.sum(raised, axis=-1, keepdims=True)) + jnp.exp(sink_col - peak_score)
        prob_bf = (raised / denominator).astype(jnp.bfloat16)
        return jnp.einsum('sgw,swh->sgh', prob_bf.astype(jnp.float32), value_part).astype(jnp.bfloat16)
    grouped = rot_queries.reshape(seq_count, kv_heads, group_size, head_size)
    attended = lax.map(attend_head, (jnp.transpose(cache_now, (1, 0, 2, 3)), jnp.transpose(grouped, (1, 0, 2, 3)), attn_sinks.reshape(kv_heads, group_size)))
    attended = jnp.transpose(attended, (1, 0, 2, 3)).reshape(seq_count, q_heads * head_size)
    residual = tok_wide + jnp.dot(attended, w_out, preferred_element_type=jnp.float32)
    moe_mean = lax.optimization_barrier(jnp.mean(residual * residual, axis=1, keepdims=True))
    scaled = residual * lax.rsqrt(moe_mean + norm_eps) * moe_gain[None, :]
    logits = jnp.dot(scaled, router.astype(jnp.float32), precision=lax.Precision.HIGHEST)
    hidden_rows = scaled.astype(jnp.bfloat16)
    experts = router.shape[1]
    expert_iota = jnp.arange(experts, dtype=jnp.int32)
    chosen = expert_ids[:, :, None] == expert_iota[None, None, :]
    picked = lax.optimization_barrier(jnp.sum(jnp.where(chosen, logits[:, None, :], 0.0), axis=-1))
    raised_logits = jnp.exp(picked)
    route_weights = raised_logits / lax.optimization_barrier(jnp.sum(raised_logits, axis=1, keepdims=True))
    per_group = seq_count // N_DP
    group_ids = expert_ids.reshape(N_DP, per_group * TOP)
    onehot = (group_ids[:, :, None] == expert_iota[None, None, :]).astype(jnp.int32)
    earlier = jnp.cumsum(onehot, axis=1) - onehot
    slot_of = lax.optimization_barrier(jnp.sum(earlier * onehot, axis=2))
    column = (jnp.arange(N_DP, dtype=jnp.int32)[:, None] * CAP + slot_of).reshape(-1).astype(jnp.int32)
    expert_flat = group_ids.reshape(-1).astype(jnp.int32)
    repeated = jnp.repeat(hidden_rows, TOP, axis=0)
    buffer_rows = jnp.zeros((experts, N_DP * CAP, full_width), jnp.bfloat16).at[expert_flat, column].set(repeated)
    ff_width = w_down.shape[1]

    def one_expert(inputs):
        block_rows, weights_in, weights_down = inputs
        mixed_in = jnp.dot(block_rows, weights_in.reshape(full_width, 2 * ff_width), preferred_element_type=jnp.float32)
        gate_part = mixed_in[:, :ff_width]
        up_part = mixed_in[:, ff_width:]
        act_rows = (gate_part * jax.nn.sigmoid(glu_alpha * gate_part) * (up_part + 1.0)).astype(jnp.bfloat16)
        return jnp.dot(act_rows, weights_down, preferred_element_type=jnp.float32).astype(jnp.bfloat16)
    outputs = lax.map(one_expert, (buffer_rows, gate_up, w_down))
    gathered = outputs[expert_flat, column].reshape(seq_count, TOP, full_width).astype(jnp.float32)
    combined = lax.optimization_barrier(jnp.sum(route_weights[:, :, None] * gathered, axis=1))
    return residual + combined
```

```python
import jax
import jax.numpy as jnp
from jax import lax
from jax.experimental import pallas as pl
from jax.experimental.pallas import tpu as pltpu
from jax.sharding import PartitionSpec as P

norm_eps = 1e-05
rope_base = 150000.0
glu_alpha = 1.702


def sent_to_all(array, axis):
    copies = jnp.broadcast_to(array, (lax.axis_size(axis), *array.shape))
    return lax.all_to_all(copies, axis, split_axis=0, concat_axis=0, tiled=True)


def taken_together(array, axis):
    everything = sent_to_all(array, axis)
    return jnp.sum(everything, axis=0)


def laid_out(parts, dim):
    parts = jnp.moveaxis(parts, 0, dim)
    shape = parts.shape
    return parts.reshape(*shape[:dim], shape[dim] * shape[dim + 1], *shape[dim + 2 :])


def gathered_copies(array, axis, dim):
    return laid_out(sent_to_all(array, axis), dim)


def in_blocks(array, dim, peers):
    shape = array.shape
    parts = array.reshape(*shape[:dim], peers, shape[dim] // peers, *shape[dim + 1 :])
    return jnp.moveaxis(parts, dim, 0)


def sum_at_owner(array, axis, dim):
    peers = lax.axis_size(axis)
    parts = lax.all_to_all(in_blocks(array, dim, peers), axis, 0, 0, tiled=True)
    return jnp.sum(parts.astype(jnp.float32), axis=0)


def rope_tables(positions, head_size):
    half_size = head_size // 2
    exponent = jnp.arange(half_size, dtype=jnp.float32) * (2.0 / head_size)
    inverse = jnp.power(jnp.float32(rope_base), -exponent)
    angles = positions.astype(jnp.float32)[:, None] * inverse[None, :]
    return (jnp.cos(angles), jnp.sin(angles))


def rotate(values, cosine, sine_table):
    half_size = values.shape[-1] // 2
    first_half = values[..., :half_size]
    second_half = values[..., half_size:]
    return jnp.concatenate(
        [
            first_half * cosine - second_half * sine_table,
            second_half * cosine + first_half * sine_table,
        ],
        axis=-1,
    )


PAD = 384
NZ = 8
NY = 4
NX = 4
SLOTS = 32
CHUNK = NY * SLOTS
WIDE = 2 * NX * PAD
MESH = pl.DeviceIdType.MESH


def z_offset(j):
    return jnp.where(lax.rem(j, 2) == 1, lax.div(j + 1, 2), NZ - lax.div(j, 2))


def experts_body(
    hid, placer, chi, clo, resid, wgu_hbm, wdn_hbm, out,
    rows, acts, wgu, wdn, placed, made, back,
    wsem, lsem, d_send, d_recv, r_send, r_recv, x_send, x_recv,
):
    dp = lax.axis_index("dp")
    tp = lax.axis_index("tp")
    z, y = lax.div(dp, NY), lax.rem(dp, NY)
    xx, core = lax.div(tp, 2), lax.rem(tp, 2)
    right = lax.rem(xx + 1, NX) * 2 + core
    left = lax.rem(xx + NX - 1, NX) * 2 + core
    across = lax.rem(xx + 2, NX) * 2 + core
    sib = xx * 2 + (1 - core)

    def flip(t):
        return t + 1 - 2 * core

    def cols(t):
        return pl.ds(pl.multiple_of(t * PAD, PAD), PAD)

    get_gu = pltpu.make_async_copy(wgu_hbm, wgu, wsem.at[0])
    get_dn = pltpu.make_async_copy(wdn_hbm, wdn, wsem.at[1])
    get_gu.start()
    get_dn.start()

    barrier = pltpu.get_barrier_semaphore()

    def greet(i, c):
        pl.semaphore_signal(
            barrier, inc=1, device_id=(lax.rem(dp + i, NZ * NY), tp), device_id_type=MESH
        )
        return c

    lax.fori_loop(1, NZ * NY, greet, 0)
    for t in (right, left, sib):
        pl.semaphore_signal(barrier, inc=1, device_id=(dp, t), device_id_type=MESH)
    pl.semaphore_wait(barrier, NZ * NY - 1 + 3)

    def dispatch_copy(j, i):
        dz = lax.rem(z + NZ - z_offset(j) , NZ)
        dest = lax.rem(dz + NZ, NZ) * NY + lax.rem(y + NY - i, NY)
        return pltpu.make_async_remote_copy(
            src_ref=placed.at[pl.ds(pl.multiple_of(dest * SLOTS, SLOTS), SLOTS), :],
            dst_ref=rows.at[j, pl.ds(pl.multiple_of(i * SLOTS, SLOTS), SLOTS), cols(tp)],
            send_sem=d_send.at[j * NY + i],
            recv_sem=d_recv.at[j * NY + i],
            device_id=(dest, tp),
            device_id_type=MESH,
        )

    own_in = pltpu.make_async_copy(
        placed.at[pl.ds(pl.multiple_of(dp * SLOTS, SLOTS), SLOTS), :],
        rows.at[0, pl.ds(0, SLOTS), cols(tp)],
        lsem.at[0],
    )

    def dispatch(j, c):
        zd = lax.rem(z + NZ - z_offset(j), NZ)
        part = pl.ds(pl.multiple_of(zd * CHUNK, CHUNK), CHUNK)
        placed[part, :] = jnp.dot(
            placer[part, :], hid[...], preferred_element_type=jnp.float32
        ).astype(jnp.bfloat16)

        @pl.when(j == 0)
        def _():
            own_in.start()

        @pl.when(j > 0)
        def _():
            dispatch_copy(j, 0).start()

        for i in range(1, NY):
            dispatch_copy(j, i).start()
        return c

    lax.fori_loop(0, NZ, dispatch, 0)

    def xcopy(buf, ph, kind, j, part, col, dest):
        ref = buf.at[j, part, cols(col)]
        return pltpu.make_async_remote_copy(
            src_ref=ref,
            dst_ref=ref,
            send_sem=x_send.at[ph, kind, j],
            recv_sem=x_recv.at[ph, kind, j],
            device_id=(dp, dest),
            device_id_type=MESH,
        )

    allr = pl.ds(0, CHUNK)
    top = pl.ds(0, CHUNK // 2)
    bot = pl.ds(CHUNK // 2, CHUNK // 2)

    def send_own(buf, ph, j):
        xcopy(buf, ph, 0, j, allr, tp, right).start()
        xcopy(buf, ph, 1, j, allr, tp, left).start()
        xcopy(buf, ph, 2, j, allr, tp, sib).start()

    def send_on(buf, ph, j):
        xcopy(buf, ph, 0, j, allr, left, right).wait_recv()
        xcopy(buf, ph, 3, j, top, left, right).start()
        xcopy(buf, ph, 4, j, allr, left, sib).start()
        xcopy(buf, ph, 1, j, allr, right, left).wait_recv()
        xcopy(buf, ph, 5, j, bot, right, left).start()
        xcopy(buf, ph, 6, j, allr, right, sib).start()

    def send_far(buf, ph, j):
        xcopy(buf, ph, 3, j, top, across, right).wait_recv()
        xcopy(buf, ph, 5, j, bot, across, left).wait_recv()
        xcopy(buf, ph, 7, j, allr, across, sib).start()

    def all_in(buf, ph, j):
        xcopy(buf, ph, 2, j, allr, sib, sib).wait_recv()
        xcopy(buf, ph, 4, j, allr, flip(left), sib).wait_recv()
        xcopy(buf, ph, 6, j, allr, flip(right), sib).wait_recv()
        xcopy(buf, ph, 7, j, allr, flip(across), sib).wait_recv()

    def back_copy(j, i):
        home = lax.rem(z + z_offset(j), NZ) * NY + lax.rem(y + i, NY)
        return pltpu.make_async_remote_copy(
            src_ref=made.at[j, pl.ds(pl.multiple_of(i * SLOTS, SLOTS), SLOTS), :],
            dst_ref=back.at[pl.ds(pl.multiple_of(dp * SLOTS, SLOTS), SLOTS), :],
            send_sem=r_send.at[j * NY + i],
            recv_sem=r_recv.at[dp],
            device_id=(home, tp),
            device_id_type=MESH,
        )

    own_back = pltpu.make_async_copy(
        made.at[0, pl.ds(0, SLOTS), :],
        back.at[pl.ds(pl.multiple_of(dp * SLOTS, SLOTS), SLOTS), :],
        lsem.at[1],
    )

    def step(t, c):
        @pl.when(t < NZ)
        def _():
            @pl.when(t == 0)
            def _():
                own_in.wait()

            @pl.when(t > 0)
            def _():
                dispatch_copy(t, 0).wait_recv()

            for i in range(1, NY):
                dispatch_copy(t, i).wait_recv()
            send_own(rows, 0, t)

        @pl.when((t >= 1) & (t < NZ + 1))
        def _():
            send_on(rows, 0, t - 1)

        @pl.when((t >= 2) & (t < NZ + 2))
        def _():
            send_far(rows, 0, t - 2)

        @pl.when(t == 3)
        def _():
            get_gu.wait()

        @pl.when((t >= 3) & (t < NZ + 3))
        def _():
            j = t - 3
            all_in(rows, 0, j)
            mixed = jnp.dot(rows[j], wgu[...], preferred_element_type=jnp.float32)
            gate = mixed[:, :PAD]
            up = mixed[:, PAD:]
            act = gate * jax.nn.sigmoid(glu_alpha * gate) * (up + 1.0)
            acts[j, :, cols(tp)] = act.astype(jnp.bfloat16)
            send_own(acts, 1, j)

        @pl.when((t >= 4) & (t < NZ + 4))
        def _():
            send_on(acts, 1, t - 4)

        @pl.when((t >= 5) & (t < NZ + 5))
        def _():
            send_far(acts, 1, t - 5)

        @pl.when(t == 6)
        def _():
            get_dn.wait()

        @pl.when(t >= 6)
        def _():
            j = t - 6
            all_in(acts, 1, j)
            made[j] = jnp.dot(acts[j], wdn[...], preferred_element_type=jnp.float32).astype(
                jnp.bfloat16
            )

            @pl.when(j == 0)
            def _():
                own_back.start()

            @pl.when(j > 0)
            def _():
                back_copy(j, 0).start()

            for i in range(1, NY):
                back_copy(j, i).start()

        return c

    lax.fori_loop(0, NZ + 6, step, 0)

    def await_back(i, c):
        peer = lax.rem(dp + i, NZ * NY)
        pltpu.make_async_remote_copy(
            src_ref=made.at[0, pl.ds(0, SLOTS), :],
            dst_ref=back.at[pl.ds(pl.multiple_of(peer * SLOTS, SLOTS), SLOTS), :],
            send_sem=r_send.at[1],
            recv_sem=r_recv.at[peer],
            device_id=(peer, tp),
            device_id_type=MESH,
        ).wait_recv()
        return c

    own_back.wait()
    lax.fori_loop(1, NZ * NY, await_back, 0)
    got = back[...]
    total = jnp.dot(chi[...], got, preferred_element_type=jnp.float32) + jnp.dot(
        clo[...], got, preferred_element_type=jnp.float32
    )
    out[...] = resid[...] + total[:, : out.shape[1]]

    def sent(n, c):
        dispatch_copy(lax.div(n, NY), lax.rem(n, NY)).wait_send()
        back_copy(lax.div(n, NY), lax.rem(n, NY)).wait_send()
        return c

    lax.fori_loop(1, NZ * NY, sent, 0)

    def sent_x(j, c):
        for ph, buf in ((0, rows), (1, acts)):
            for kind in range(8):
                part = top if kind == 3 else bot if kind == 5 else allr
                xcopy(buf, ph, kind, j, part, tp, right).wait_send()
        return c

    lax.fori_loop(0, NZ, sent_x, 0)


def experts_kernel(hid, placer, chi, clo, resid, wgu, wdn):
    vmem = pl.BlockSpec(memory_space=pltpu.VMEM)
    hbm = pl.BlockSpec(memory_space=pl.ANY)
    dma = pltpu.SemaphoreType.DMA
    bf = jnp.bfloat16
    return pl.pallas_call(
        experts_body,
        out_shape=jax.ShapeDtypeStruct(resid.shape, jnp.float32),
        in_specs=[vmem] * 5 + [hbm] * 2,
        out_specs=vmem,
        scratch_shapes=[
            pltpu.VMEM((NZ, CHUNK, WIDE), bf),
            pltpu.VMEM((NZ, CHUNK, WIDE), bf),
            pltpu.VMEM((WIDE, 2 * PAD), bf),
            pltpu.VMEM((WIDE, PAD), bf),
            pltpu.VMEM((NZ * CHUNK, PAD), bf),
            pltpu.VMEM((NZ, CHUNK, PAD), bf),
            pltpu.VMEM((NZ * CHUNK, PAD), bf),
            dma((2,)),
            dma((2,)),
            dma((NZ * NY,)),
            dma((NZ * NY,)),
            dma((NZ * NY,)),
            dma((NZ * NY,)),
            dma((2, 8, NZ)),
            dma((2, 8, NZ)),
        ],
        compiler_params=pltpu.CompilerParams(
            collective_id=0, has_side_effects=True, vmem_limit_bytes=48 * 1024 * 1024
        ),
        name="experts",
    )(hid, placer, chi, clo, resid, wgu, wdn)


def on_device(
    tokens,
    attn_gain,
    w_query,
    w_keyvalue,
    attn_sinks,
    w_out,
    window_cache,
    positions,
    moe_gain,
    router,
    gate_up,
    w_down,
    expert_ids,
):
    tp_count = lax.axis_size("tp")
    dp_count = lax.axis_size("dp")
    seq_count, col_count = tokens.shape
    full_width = col_count * tp_count
    col_start = lax.axis_index("tp") * col_count
    head_size = w_keyvalue.shape[2] // 2
    kv_local = w_keyvalue.shape[1]
    q_local = w_query.shape[1] // head_size
    group_size = q_local // kv_local
    window = window_cache.shape[2]
    attn_slice = lax.dynamic_slice_in_dim(attn_gain, col_start, col_count)
    moe_slice = lax.dynamic_slice_in_dim(moe_gain, col_start, col_count)
    tok_wide = tokens.astype(jnp.float32)
    attn_sq = taken_together(jnp.sum(tok_wide * tok_wide, axis=1), "tp")
    normed = (
        tok_wide * lax.rsqrt(attn_sq / full_width + norm_eps)[:, None] * attn_slice[None, :]
    ).astype(jnp.bfloat16)
    kv_flat = w_keyvalue.reshape(full_width, kv_local * 2 * head_size)
    piece_rows = gathered_copies(normed, "tp", 1)
    queries = jnp.dot(piece_rows, w_query, preferred_element_type=jnp.float32)
    fresh_rows = jnp.dot(piece_rows, kv_flat, preferred_element_type=jnp.float32)
    cosine, sine_table = rope_tables(positions, head_size)
    rot_queries = rotate(
        queries.reshape(seq_count, q_local, head_size), cosine[:, None, :], sine_table[:, None, :]
    ).astype(jnp.bfloat16)
    fresh_rows = fresh_rows.reshape(seq_count, kv_local, 2 * head_size)
    new_key = rotate(fresh_rows[..., :head_size], cosine[:, None, :], sine_table[:, None, :])
    new_entry = jnp.concatenate([new_key, fresh_rows[..., head_size:]], axis=-1).astype(
        jnp.bfloat16
    )
    slot_ids = jnp.arange(window, dtype=jnp.int32)
    is_current = slot_ids[None, :] == (positions % window)[:, None]
    cache_now = jnp.where(is_current[:, None, :, None], new_entry[:, :, None, :], window_cache)
    is_valid = (positions[:, None] - slot_ids[None, :]) % window <= positions[:, None]
    grouped = rot_queries.reshape(seq_count, kv_local, group_size, head_size)
    scores = jnp.einsum(
        "skgh,skwh->skgw", grouped, cache_now[..., :head_size], preferred_element_type=jnp.float32
    ) * head_size ** (-0.5)
    scores = jnp.where(is_valid[:, None, None, :], scores, -jnp.inf)
    sink_col = attn_sinks.reshape(kv_local, group_size)[None, :, :, None]
    peak_score = jnp.maximum(jnp.max(scores, axis=-1, keepdims=True), sink_col)
    raised = jnp.exp(scores - peak_score)
    denominator = jnp.sum(raised, axis=-1, keepdims=True) + jnp.exp(sink_col - peak_score)
    prob_bf = (raised / denominator).astype(jnp.bfloat16)
    attended = jnp.einsum(
        "skgw,skwh->skgh", prob_bf, cache_now[..., head_size:], preferred_element_type=jnp.float32
    ).astype(jnp.bfloat16)
    partial_out = jnp.dot(
        attended.reshape(seq_count, q_local * head_size), w_out, preferred_element_type=jnp.float32
    )
    residual = tok_wide + sum_at_owner(partial_out.astype(jnp.bfloat16), "tp", 1)
    experts = router.shape[1]
    top_count = expert_ids.shape[1]
    local_experts = gate_up.shape[0]
    ff_local = gate_up.shape[3]
    capacity = min(seq_count, max(2, 8 * seq_count * top_count // (3 * experts)))
    moe_sq = jnp.sum(residual * residual, axis=1)
    router_wide = router.astype(jnp.float32)
    total_sq = taken_together(moe_sq, "tp")
    moe_scale = lax.rsqrt(total_sq / full_width + norm_eps)[:, None]
    scaled = residual * moe_scale * moe_slice[None, :]
    logits = taken_together(jnp.dot(scaled, router_wide, precision=lax.Precision.HIGHEST), "tp")
    hidden_rows = scaled.astype(jnp.bfloat16)
    expert_iota = jnp.arange(experts, dtype=jnp.int32)
    chosen = expert_ids[:, :, None] == expert_iota[None, None, :]
    picked = jnp.sum(jnp.where(chosen, logits[:, None, :], 0.0), axis=-1)
    raised_logits = jnp.exp(picked)
    route_weights = raised_logits / jnp.sum(raised_logits, axis=1, keepdims=True)
    assign = expert_ids.reshape(-1)
    onehot = (assign[:, None] == expert_iota[None, :]).astype(jnp.int32)
    earlier = jnp.cumsum(onehot, axis=0) - onehot
    slot_of = jnp.sum(earlier * onehot, axis=1)
    target = (assign * capacity + slot_of).reshape(seq_count, top_count)
    spot_ids = jnp.arange(experts * capacity, dtype=jnp.int32)
    slot_hits = target[:, :, None] == spot_ids[None, None, :]
    placer = jnp.transpose(jnp.any(slot_hits, axis=1)).astype(jnp.bfloat16)
    combiner = jnp.sum(jnp.where(slot_hits, route_weights[:, :, None], 0.0), axis=1)
    comb_hi = combiner.astype(jnp.bfloat16)
    comb_lo = (combiner - comb_hi.astype(jnp.float32)).astype(jnp.bfloat16)
    hidden_pad = jnp.pad(hidden_rows, ((0, 0), (0, PAD - col_count)))
    wgu = jnp.pad(
        gate_up.reshape(tp_count, col_count, 2, ff_local),
        ((0, 0), (0, PAD - col_count), (0, 0), (0, PAD - ff_local)),
    ).reshape(tp_count * PAD, 2 * PAD)
    wdn = jnp.pad(
        w_down.reshape(tp_count, ff_local, col_count),
        ((0, 0), (0, PAD - ff_local), (0, PAD - col_count)),
    ).reshape(tp_count * PAD, PAD)
    return experts_kernel(hidden_pad, placer, comb_hi, comb_lo, residual, wgu, wdn)


def solution(mesh):
    in_specs = (
        P("dp", "tp"),
        P(),
        P(None, "tp"),
        P(None, "tp", None),
        P("tp"),
        P("tp", None),
        P("dp", "tp", None, None),
        P("dp"),
        P(),
        P("tp", None),
        P("dp", None, None, "tp"),
        P("dp", None, "tp"),
        P("dp", None),
    )
    out_specs = P("dp", "tp")
    return jax.shard_map(
        on_device, mesh=mesh, in_specs=in_specs, out_specs=out_specs, check_vma=False
    )
```

```python
import math

import jax
import jax.numpy as jnp
from jax import lax
from jax.experimental import pallas as pl
from jax.experimental.pallas import tpu as pltpu
from jax.sharding import PartitionSpec as P

norm_eps = 1e-05
rope_base = 150000.0
glu_alpha = 1.702

COL = 360
PAD = 384
FULL = 2880
NZ = 8
NY = 4
NX = 4
NTP = 2 * NX
SLOTS = 32
CHUNK = NY * SLOTS
WIDE = NTP * PAD
TOK = 96
HEADS = 4
HD = 64
LANES = 128
SPAN = 8 * TOK
MESH = pl.DeviceIdType.MESH
NT = (((1,), (1,)), ((), ()))
F32 = jnp.float32
BF = jnp.bfloat16


def z_offset(j):
    return jnp.where(lax.rem(j, 2) == 1, lax.div(j + 1, 2), NZ - lax.div(j, 2))


def dot_nt(a, b):
    return lax.dot_general(a, b, NT, preferred_element_type=F32)


def split3(v):
    hi = v.astype(BF)
    rest = v - hi.astype(F32)
    mid = rest.astype(BF)
    low = (rest - mid.astype(F32)).astype(BF)
    return hi, mid, low


def spread_blocks(src, dst, rows, row_step):
    def part(n, c):
        at = pl.ds(pl.multiple_of(n * row_step, row_step), row_step)
        for b in range(NTP):
            low = b * COL // LANES * LANES
            off = b * COL - low
            high = min(low + 4 * LANES, FULL)
            piece = src[at, low:high]
            dst[at, b * PAD + 2 * LANES : (b + 1) * PAD] = jnp.zeros((row_step, LANES), dst.dtype)
            dst[at, b * PAD : b * PAD + COL] = piece[:, off : off + COL]
        return c

    lax.fori_loop(0, rows // row_step, part, 0)


def layer_body(
    tokens, again, mgain, sinks, pos, router_t, ids_t,
    wq_hbm, wkv_hbm, wo_hbm, cache_hbm, gu_hbm, dn_hbm,
    out,
    rows, acts, wgu, wdn, placed, made, back,
    toks, wq, wkv, wo, cache, raw_gu, raw_dn,
    gain_pad, own_gain, tok_pad, qbuf, kvb, scb, resid, hid, placer, comb_hi, comb_lo,
    mine_f, mine_b, sib_b, chip_b, recv_b, table, small, small_t,
    wsem, lsem, d_send, d_recv, r_send, r_recv, x_send, x_recv,
    o_send, o_recv, a_send, a_recv,
):
    dp = lax.axis_index("dp")
    tp = lax.axis_index("tp")
    z, y = lax.div(dp, NY), lax.rem(dp, NY)
    xx, core = lax.div(tp, 2), lax.rem(tp, 2)
    right = lax.rem(xx + 1, NX) * 2 + core
    left = lax.rem(xx + NX - 1, NX) * 2 + core
    across = lax.rem(xx + 2, NX) * 2 + core
    sib = xx * 2 + (1 - core)

    def flip(t):
        return t + 1 - 2 * core

    def cols(t):
        return pl.ds(pl.multiple_of(t * PAD, PAD), PAD)

    barrier = pltpu.get_barrier_semaphore()

    def greet(i, c):
        pl.semaphore_signal(
            barrier, inc=1, device_id=(lax.rem(dp + i, NZ * NY), tp), device_id_type=MESH
        )
        return c

    def greet_tp(i, c):
        pl.semaphore_signal(
            barrier, inc=1, device_id=(dp, lax.rem(tp + i, NTP)), device_id_type=MESH
        )
        return c

    lax.fori_loop(1, NTP, greet_tp, 0)
    lax.fori_loop(1, NZ * NY, greet, 0)

    get_q = [
        pltpu.make_async_copy(
            wq_hbm.at[pl.ds(b * COL, COL), :], wq.at[pl.ds(b * PAD, COL), :], wsem.at[b]
        )
        for b in range(NTP)
    ]
    get_kv = [
        pltpu.make_async_copy(
            wkv_hbm.at[pl.ds(b * COL, COL), :], wkv.at[pl.ds(b * PAD, COL), :], wsem.at[8 + b]
        )
        for b in range(NTP)
    ]
    get_o = [
        pltpu.make_async_copy(
            wo_hbm.at[pl.ds(b * COL, COL), :], wo.at[pl.ds(b * PAD, COL), :], wsem.at[16 + b]
        )
        for b in range(NTP)
    ]
    get_cache = pltpu.make_async_copy(cache_hbm, cache, wsem.at[24])
    get_gu = [
        pltpu.make_async_copy(gu_hbm.at[u], raw_gu.at[pl.ds(u * PAD, COL), :], wsem.at[25 + u])
        for u in range(2)
    ]
    get_dn = pltpu.make_async_copy(dn_hbm, raw_dn.at[pl.ds(0, COL), :], wsem.at[27])
    for group in (get_gu, [get_dn], get_q, get_kv, [get_cache], get_o):
        for get in group:
            get.start()

    tok_pad[...] = jnp.zeros((TOK, PAD), F32)
    tok_pad[:, :COL] = tokens[...].astype(F32)
    toks[0, :, cols(tp)] = tok_pad[...].astype(BF)

    def xcopy(buf, ph, kind, j, part, col, dest):
        ref = buf.at[j, part, cols(col)]
        return pltpu.make_async_remote_copy(
            src_ref=ref,
            dst_ref=ref,
            send_sem=x_send.at[ph, kind, j],
            recv_sem=x_recv.at[ph, kind, j],
            device_id=(dp, dest),
            device_id_type=MESH,
        )

    def parts_of(buf):
        n = buf.shape[1]
        return pl.ds(0, n), pl.ds(0, n // 2), pl.ds(n // 2, n // 2)

    def send_own(buf, ph, j):
        allr, top, bot = parts_of(buf)
        xcopy(buf, ph, 0, j, allr, tp, right).start()
        xcopy(buf, ph, 1, j, allr, tp, left).start()
        xcopy(buf, ph, 2, j, allr, tp, sib).start()

    def send_on(buf, ph, j):
        allr, top, bot = parts_of(buf)
        xcopy(buf, ph, 0, j, allr, left, right).wait_recv()
        xcopy(buf, ph, 3, j, top, left, right).start()
        xcopy(buf, ph, 4, j, allr, left, sib).start()
        xcopy(buf, ph, 1, j, allr, right, left).wait_recv()
        xcopy(buf, ph, 5, j, bot, right, left).start()
        xcopy(buf, ph, 6, j, allr, right, sib).start()

    def send_far(buf, ph, j):
        allr, top, bot = parts_of(buf)
        xcopy(buf, ph, 3, j, top, across, right).wait_recv()
        xcopy(buf, ph, 5, j, bot, across, left).wait_recv()
        xcopy(buf, ph, 7, j, allr, across, sib).start()

    def all_in(buf, ph, j):
        allr, top, bot = parts_of(buf)
        xcopy(buf, ph, 2, j, allr, sib, sib).wait_recv()
        xcopy(buf, ph, 4, j, allr, flip(left), sib).wait_recv()
        xcopy(buf, ph, 6, j, allr, flip(right), sib).wait_recv()
        xcopy(buf, ph, 7, j, allr, flip(across), sib).wait_recv()

    def all_sent(buf, ph, j):
        allr, top, bot = parts_of(buf)
        for kind in range(8):
            part = top if kind == 3 else bot if kind == 5 else allr
            xcopy(buf, ph, kind, j, part, tp, right).wait_send()

    pl.semaphore_wait(barrier, NZ * NY - 1 + NTP - 1)
    send_own(toks, 2, 0)

    for b in range(NTP):
        gain_pad[:, b * PAD + 2 * LANES : (b + 1) * PAD] = jnp.zeros((1, LANES), F32)
        gain_pad[:, b * PAD : b * PAD + COL] = again[:, b * COL : (b + 1) * COL]
        own = mgain[:, b * COL : (b + 1) * COL]

        @pl.when(tp == b)
        def _():
            own_gain[...] = jnp.zeros((1, PAD), F32)
            own_gain[:, :COL] = own

    small[...] = jnp.zeros((8, LANES), F32)
    small[0:1, :TOK] = pos[...].astype(F32)
    pos_col = jnp.transpose(jnp.broadcast_to(small[0:1, :], (LANES, LANES)))[:TOK]
    lane = lax.broadcasted_iota(jnp.int32, (TOK, LANES), 1)
    inverse = jnp.exp(
        lax.rem(lane, HD // 2).astype(F32) * (-2.0 / HD * math.log(rope_base))
    )
    angles = pos_col * inverse
    first = lax.rem(lane, HD) < HD // 2
    table[0] = jnp.cos(angles)
    sine = jnp.sin(angles)
    table[1] = jnp.where(first, -sine, sine)
    table[2] = pos_col

    experts = NZ * NY
    e_iota = lax.broadcasted_iota(jnp.int32, (experts, TOK), 0)
    named = e_iota == ids_t[0:1, :]
    for k in range(1, ids_t.shape[0]):
        named = named | (e_iota == ids_t[k : k + 1, :])
    before = (
        lax.broadcasted_iota(jnp.int32, (TOK, TOK), 0)
        < lax.broadcasted_iota(jnp.int32, (TOK, TOK), 1)
    ).astype(F32)
    named_f = named.astype(F32)
    slot = jnp.dot(named_f, before, preferred_element_type=F32)
    slot = jnp.where(named, slot, -1.0)
    s_iota = lax.broadcasted_iota(jnp.int32, (SLOTS, TOK), 0).astype(F32)
    for e in range(experts):
        placer[e * SLOTS : (e + 1) * SLOTS, :] = (
            s_iota == slot[e : e + 1, :]
        ).astype(F32)

    send_on(toks, 2, 0)
    for u, get in enumerate(get_gu):
        get.wait()
    raw_gu[COL:PAD, :] = jnp.zeros((PAD - COL, FULL), BF)
    raw_gu[PAD + COL : 2 * PAD, :] = jnp.zeros((PAD - COL, FULL), BF)
    spread_blocks(raw_gu, wgu, 2 * PAD, 48)
    send_far(toks, 2, 0)
    get_dn.wait()
    raw_dn[COL:PAD, :] = jnp.zeros((PAD - COL, FULL), BF)
    spread_blocks(raw_dn, wdn, PAD, 48)
    for group, ref in ((get_q, wq), (get_kv, wkv), (get_o, wo)):
        for b, get in enumerate(group):
            get.wait()
            ref[b * PAD + COL : (b + 1) * PAD, :] = jnp.zeros((PAD - COL, ref.shape[1]), BF)
    all_in(toks, 2, 0)

    wide = toks[0].astype(F32)
    mean = jnp.sum(wide * wide, axis=1, keepdims=True) * (1.0 / FULL)
    normed = (wide * lax.rsqrt(mean + norm_eps) * gain_pad[...]).astype(BF)
    queries = jnp.dot(normed, wq[...], preferred_element_type=F32)
    fresh = jnp.dot(normed, wkv[...], preferred_element_type=F32)

    def turned(v):
        swapped = jnp.where(
            first, pltpu.roll(v, LANES - HD // 2, axis=1), pltpu.roll(v, HD // 2, axis=1)
        )
        return v * table[0] + swapped * table[1]

    entry = jnp.where(lane < HD, turned(fresh), fresh).astype(BF).astype(F32)
    qbuf[...] = jnp.zeros((SPAN, LANES), F32)
    kvb[...] = jnp.zeros((SPAN, LANES), F32)
    for g in range(HEADS):
        tile = g // 2
        if g % 2 == 0:
            rotated = turned(queries[:, tile * LANES : (tile + 1) * LANES]).astype(BF).astype(F32)
        head = rotated if g % 2 == 0 else pltpu.roll(rotated, HD, axis=1)
        qbuf[pl.ds(g, TOK, stride=8), :] = jnp.where(lane < HD, head * HD**-0.5, 0.0)
        kvb[pl.ds(g, TOK, stride=8), :] = entry
    get_cache.wait()

    def score(n, c):
        for u in range(8):
            s = n * 8 + u
            at = pl.ds(pl.multiple_of(s * 8, 8), 8)
            scb[at, :] = dot_nt(qbuf[at, :].astype(BF), cache[s])
        return c

    lax.fori_loop(0, TOK // 8, score, 0)
    sub = lax.broadcasted_iota(jnp.int32, (8, LANES), 0)
    sink = jnp.where(
        sub == 0,
        sinks[0],
        jnp.where(sub == 1, sinks[1], jnp.where(sub == 2, sinks[2], sinks[3])),
    )[:, :1]
    slots = lax.broadcasted_iota(jnp.int32, (8, LANES), 1)

    def soften(n, c):
        for u in range(8):
            s = n * 8 + u
            at = pl.ds(pl.multiple_of(s * 8, 8), 8)
            where_now = table[2, pl.ds(s, 1), :].astype(jnp.int32)
            current = slots == lax.rem(where_now, LANES)
            newest = jnp.sum(qbuf[at, :] * kvb[at, :], axis=1, keepdims=True)
            raw = jnp.where(current, newest, scb[at, :])
            raw = jnp.where(slots <= where_now, raw, -jnp.inf)
            peak = jnp.maximum(jnp.max(raw, axis=1, keepdims=True), sink)
            raised = jnp.exp(raw - peak)
            total = jnp.sum(raised, axis=1, keepdims=True) + jnp.exp(sink - peak)
            probs = (raised / total).astype(BF)
            newest_prob = (jnp.exp(newest - peak) / total).astype(BF).astype(F32)
            kept = jnp.where(current, 0.0, probs.astype(F32)).astype(BF)
            mixed = jnp.dot(kept, cache[s], preferred_element_type=F32)
            scb[at, :] = mixed + newest_prob * kvb[at, :]
        return c

    lax.fori_loop(0, TOK // 8, soften, 0)
    tiles = []
    for tile in range(2):
        even = scb[pl.ds(2 * tile, TOK, stride=8), :]
        odd = scb[pl.ds(2 * tile + 1, TOK, stride=8), :]
        tiles.append(jnp.where(lane < HD, pltpu.roll(even, HD, axis=1), odd).astype(BF))
    attended = jnp.concatenate(tiles, axis=1)

    def out_block(owner):
        return dot_nt(attended, wo[cols(owner), :])

    for n in range(NX):
        mine_b[n] = out_block(2 * n + 1 - core).astype(BF)
    to_sib = pltpu.make_async_remote_copy(
        src_ref=mine_b,
        dst_ref=sib_b,
        send_sem=o_send.at[0],
        recv_sem=o_recv.at[0],
        device_id=(dp, sib),
        device_id_type=MESH,
    )
    to_sib.start()
    for n in range(NX):
        mine_f[n] = out_block(2 * n + core)
    to_sib.wait_recv()

    def to_chip(i):
        owner = lax.rem(xx + i, NX)
        return pltpu.make_async_remote_copy(
            src_ref=chip_b.at[owner],
            dst_ref=recv_b.at[i],
            send_sem=o_send.at[i],
            recv_sem=o_recv.at[i],
            device_id=(dp, owner * 2 + core),
            device_id_type=MESH,
        )

    for i in (2, 1, 3):
        owner = lax.rem(xx + i, NX)
        chip_b[owner] = (mine_f[owner] + sib_b[owner].astype(F32)).astype(BF)
        to_chip(i).start()
    total = tok_pad[...] + (mine_f[xx] + sib_b[xx].astype(F32))
    for i in (1, 3, 2):
        to_chip(i).wait_recv()
    for i in (1, 2, 3):
        total = total + recv_b[i].astype(F32)
    resid[...] = total

    lifted = total * own_gain[...]
    wide_rows = jnp.zeros((LANES - TOK, PAD), BF)
    logit_part = jnp.zeros((experts, LANES), F32)
    for piece in split3(lifted):
        logit_part = logit_part + dot_nt(router_t[...], jnp.concatenate([piece, wide_rows], axis=0))
    square_part = jnp.zeros((8, LANES), F32)
    ones = jnp.ones((8, PAD), BF)
    for piece in split3(total * total):
        square_part = square_part + dot_nt(ones, jnp.concatenate([piece, wide_rows], axis=0))
    small_t[tp, 0:experts, :] = logit_part
    small_t[tp, experts : experts + 8, :] = square_part

    def share(i):
        return pltpu.make_async_remote_copy(
            src_ref=small_t.at[tp],
            dst_ref=small_t.at[tp],
            send_sem=a_send.at[i],
            recv_sem=a_recv.at[i],
            device_id=(dp, lax.rem(tp + i, NTP)),
            device_id_type=MESH,
        )

    for i in range(1, NTP):
        share(i).start()
    for i in range(1, NTP):
        share(i).wait_recv()
    summed = small_t[0]
    for n in range(1, NTP):
        summed = summed + small_t[n]
    scale_row = lax.rsqrt(summed[experts : experts + 1, :] * (1.0 / FULL) + norm_eps)
    scale_col = jnp.transpose(jnp.broadcast_to(scale_row, (LANES, LANES)))[:TOK, :1]
    hid[...] = (resid[...] * scale_col * own_gain[...]).astype(BF)

    def dispatch_copy(j, i):
        dest = lax.rem(z + NZ + NZ - z_offset(j), NZ) * NY + lax.rem(y + NY - i, NY)
        return pltpu.make_async_remote_copy(
            src_ref=placed.at[pl.ds(pl.multiple_of(dest * SLOTS, SLOTS), SLOTS), :],
            dst_ref=rows.at[j, pl.ds(pl.multiple_of(i * SLOTS, SLOTS), SLOTS), cols(tp)],
            send_sem=d_send.at[j * NY + i],
            recv_sem=d_recv.at[j * NY + i],
            device_id=(dest, tp),
            device_id_type=MESH,
        )

    own_in = pltpu.make_async_copy(
        placed.at[pl.ds(pl.multiple_of(dp * SLOTS, SLOTS), SLOTS), :],
        rows.at[0, pl.ds(0, SLOTS), cols(tp)],
        lsem.at[0],
    )

    def dispatch(j, c):
        zd = lax.rem(z + NZ + NZ - z_offset(j), NZ)
        part = pl.ds(pl.multiple_of(zd * CHUNK, CHUNK), CHUNK)
        placed[part, :] = jnp.dot(
            placer[part, :].astype(BF), hid[...], preferred_element_type=F32
        ).astype(BF)

        @pl.when(j == 0)
        def _():
            own_in.start()

        @pl.when(j > 0)
        def _():
            dispatch_copy(j, 0).start()

        for i in range(1, NY):
            dispatch_copy(j, i).start()
        return c

    lax.fori_loop(0, NZ, dispatch, 0)

    logits = summed[0:experts, :TOK] * scale_row[:, :TOK]
    lifted_logits = jnp.where(named, jnp.exp(logits), 0.0)
    weights = lifted_logits / jnp.sum(lifted_logits, axis=0, keepdims=True)
    for e in range(experts):
        at = slice(e * SLOTS, (e + 1) * SLOTS)
        placer[at, :] = placer[at, :] * weights[e : e + 1, :]
    for n in range(NZ):
        at = slice(n * CHUNK, (n + 1) * CHUNK)
        piece = jnp.transpose(placer[at, :])
        hi = piece.astype(BF)
        comb_hi[:, at] = hi
        comb_lo[:, at] = (piece - hi.astype(F32)).astype(BF)

    def back_copy(j, i):
        home = lax.rem(z + z_offset(j), NZ) * NY + lax.rem(y + i, NY)
        return pltpu.make_async_remote_copy(
            src_ref=made.at[j, pl.ds(pl.multiple_of(i * SLOTS, SLOTS), SLOTS), :],
            dst_ref=back.at[pl.ds(pl.multiple_of(dp * SLOTS, SLOTS), SLOTS), :],
            send_sem=r_send.at[j * NY + i],
            recv_sem=r_recv.at[dp],
            device_id=(home, tp),
            device_id_type=MESH,
        )

    own_back = pltpu.make_async_copy(
        made.at[0, pl.ds(0, SLOTS), :],
        back.at[pl.ds(pl.multiple_of(dp * SLOTS, SLOTS), SLOTS), :],
        lsem.at[1],
    )

    def step(t, c):
        @pl.when(t < NZ)
        def _():
            @pl.when(t == 0)
            def _():
                own_in.wait()

            @pl.when(t > 0)
            def _():
                dispatch_copy(t, 0).wait_recv()

            for i in range(1, NY):
                dispatch_copy(t, i).wait_recv()
            send_own(rows, 0, t)

        @pl.when((t >= 1) & (t < NZ + 1))
        def _():
            send_on(rows, 0, t - 1)

        @pl.when((t >= 2) & (t < NZ + 2))
        def _():
            send_far(rows, 0, t - 2)

        @pl.when((t >= 3) & (t < NZ + 3))
        def _():
            j = t - 3
            all_in(rows, 0, j)
            mixed = dot_nt(rows[j], wgu[...])
            gate = mixed[:, :PAD]
            up = mixed[:, PAD:]
            act = gate * jax.nn.sigmoid(glu_alpha * gate) * (up + 1.0)
            acts[j, :, cols(tp)] = act.astype(BF)
            send_own(acts, 1, j)

        @pl.when((t >= 4) & (t < NZ + 4))
        def _():
            send_on(acts, 1, t - 4)

        @pl.when((t >= 5) & (t < NZ + 5))
        def _():
            send_far(acts, 1, t - 5)

        @pl.when(t >= 6)
        def _():
            j = t - 6
            all_in(acts, 1, j)
            made[j] = dot_nt(acts[j], wdn[...]).astype(BF)

            @pl.when(j == 0)
            def _():
                own_back.start()

            @pl.when(j > 0)
            def _():
                back_copy(j, 0).start()

            for i in range(1, NY):
                back_copy(j, i).start()

        return c

    lax.fori_loop(0, NZ + 6, step, 0)

    def await_back(i, c):
        peer = lax.rem(dp + i, NZ * NY)
        pltpu.make_async_remote_copy(
            src_ref=made.at[0, pl.ds(0, SLOTS), :],
            dst_ref=back.at[pl.ds(pl.multiple_of(peer * SLOTS, SLOTS), SLOTS), :],
            send_sem=r_send.at[1],
            recv_sem=r_recv.at[peer],
            device_id=(peer, tp),
            device_id_type=MESH,
        ).wait_recv()
        return c

    own_back.wait()
    lax.fori_loop(1, NZ * NY, await_back, 0)
    got = back[...]
    answer = (
        resid[...]
        + jnp.dot(comb_hi[...], got, preferred_element_type=F32)
        + jnp.dot(comb_lo[...], got, preferred_element_type=F32)
    )
    out[...] = answer[:, :COL]

    to_sib.wait_send()
    for i in range(1, NX):
        to_chip(i).wait_send()
    for i in range(1, NTP):
        share(i).wait_send()
    all_sent(toks, 2, 0)

    def sent(n, c):
        dispatch_copy(lax.div(n, NY), lax.rem(n, NY)).wait_send()
        back_copy(lax.div(n, NY), lax.rem(n, NY)).wait_send()
        return c

    lax.fori_loop(1, NZ * NY, sent, 0)

    def sent_x(j, c):
        all_sent(rows, 0, j)
        all_sent(acts, 1, j)
        return c

    lax.fori_loop(0, NZ, sent_x, 0)


def on_device(
    tokens,
    attn_gain,
    w_query,
    w_keyvalue,
    attn_sinks,
    w_out,
    window_cache,
    positions,
    moe_gain,
    router,
    gate_up,
    w_down,
    expert_ids,
):
    vmem = pl.BlockSpec(memory_space=pltpu.VMEM)
    smem = pl.BlockSpec(memory_space=pltpu.SMEM)
    hbm = pl.BlockSpec(memory_space=pl.ANY)
    dma = pltpu.SemaphoreType.DMA
    vm = pltpu.VMEM
    router_t = jnp.pad(jnp.transpose(router), ((0, 0), (0, PAD - COL)))
    return pl.pallas_call(
        layer_body,
        out_shape=jax.ShapeDtypeStruct(tokens.shape, F32),
        in_specs=[vmem, vmem, vmem, smem, vmem, vmem, vmem] + [hbm] * 6,
        out_specs=vmem,
        scratch_shapes=[
            vm((NZ, CHUNK, WIDE), BF),
            vm((NZ, CHUNK, WIDE), BF),
            vm((2 * PAD, WIDE), BF),
            vm((PAD, WIDE), BF),
            vm((NZ * CHUNK, PAD), BF),
            vm((NZ, CHUNK, PAD), BF),
            vm((NZ * CHUNK, PAD), BF),
            vm((1, TOK, WIDE), BF),
            vm((WIDE, HEADS * HD), BF),
            vm((WIDE, 2 * HD), BF),
            vm((WIDE, HEADS * HD), BF),
            vm((TOK, LANES, 2 * HD), BF),
            vm((2 * PAD, FULL), BF),
            vm((PAD, FULL), BF),
            vm((1, WIDE), F32),
            vm((1, PAD), F32),
            vm((TOK, PAD), F32),
            vm((SPAN, LANES), F32),
            vm((SPAN, LANES), F32),
            vm((SPAN, LANES), F32),
            vm((TOK, PAD), F32),
            vm((TOK, PAD), BF),
            vm((NZ * CHUNK, TOK), F32),
            vm((TOK, NZ * CHUNK), BF),
            vm((TOK, NZ * CHUNK), BF),
            vm((NX, TOK, PAD), F32),
            vm((NX, TOK, PAD), BF),
            vm((NX, TOK, PAD), BF),
            vm((NX, TOK, PAD), BF),
            vm((NX, TOK, PAD), BF),
            vm((3, TOK, LANES), F32),
            vm((8, LANES), F32),
            vm((NTP, 40, LANES), F32),
            dma((28,)),
            dma((2,)),
            dma((NZ * NY,)),
            dma((NZ * NY,)),
            dma((NZ * NY,)),
            dma((NZ * NY,)),
            dma((3, 8, NZ)),
            dma((3, 8, NZ)),
            dma((NX,)),
            dma((NX,)),
            dma((NTP,)),
            dma((NTP,)),
        ],
        compiler_params=pltpu.CompilerParams(
            collective_id=0, has_side_effects=True, vmem_limit_bytes=60 * 1024 * 1024
        ),
        name="layer",
    )(
        tokens,
        attn_gain[None, :],
        moe_gain[None, :],
        attn_sinks,
        positions[None, :],
        router_t,
        jnp.transpose(expert_ids),
        w_query,
        w_keyvalue.reshape(FULL, 2 * HD),
        jnp.transpose(w_out),
        window_cache.reshape(TOK, LANES, 2 * HD),
        jnp.transpose(gate_up[0], (1, 2, 0)),
        jnp.transpose(w_down[0]),
    )


def solution(mesh):
    in_specs = (
        P("dp", "tp"),
        P(),
        P(None, "tp"),
        P(None, "tp", None),
        P("tp"),
        P("tp", None),
        P("dp", "tp", None, None),
        P("dp"),
        P(),
        P("tp", None),
        P("dp", None, None, "tp"),
        P("dp", None, "tp"),
        P("dp", None),
    )
    out_specs = P("dp", "tp")
    return jax.shard_map(
        on_device, mesh=mesh, in_specs=in_specs, out_specs=out_specs, check_vma=False
    )
```

```python
import math

import jax
import jax.numpy as jnp
from jax import lax
from jax.experimental import pallas as pl
from jax.experimental.pallas import tpu as pltpu
from jax.sharding import PartitionSpec as P

norm_eps = 1e-05
rope_base = 150000.0
glu_alpha = 1.702

COL = 360
PAD = 384
FULL = 2880
NZ = 8
NY = 4
NX = 4
NTP = 2 * NX
SLOTS = 32
CHUNK = NY * SLOTS
WIDE = NTP * PAD
TOK = 96
HEADS = 4
HD = 64
LANES = 128
SPAN = 8 * TOK
MESH = pl.DeviceIdType.MESH
NT = (((1,), (1,)), ((), ()))
F32 = jnp.float32
BF = jnp.bfloat16


ORDER = (0, 7, 2, 4, 5, 3, 6, 1)
OWN = ORDER.index(0)
AHEAD = 3
STRAIGHT_ROWS = 1
STRAIGHT_ACTS = 2
STRAIGHT_TOKENS = True


def z_offset(j):
    offset = 0
    for n, value in enumerate(ORDER):
        offset = jnp.where(j == n, value, offset)
    return offset


def dot_nt(a, b):
    return lax.dot_general(a, b, NT, preferred_element_type=F32)


def split3(v):
    hi = v.astype(BF)
    rest = v - hi.astype(F32)
    mid = rest.astype(BF)
    low = (rest - mid.astype(F32)).astype(BF)
    return hi, mid, low


def spread_blocks(src, dst, rows, row_step):
    def part(n, c):
        at = pl.ds(pl.multiple_of(n * row_step, row_step), row_step)
        for b in range(NTP):
            low = b * COL // LANES * LANES
            off = b * COL - low
            high = min(low + 4 * LANES, FULL)
            piece = src[at, low:high]
            dst[at, b * PAD + 2 * LANES : (b + 1) * PAD] = jnp.zeros((row_step, LANES), dst.dtype)
            dst[at, b * PAD : b * PAD + COL] = piece[:, off : off + COL]
        return c

    lax.fori_loop(0, rows // row_step, part, 0)


def layer_body(
    tokens, gains, sinks, pos, router_t, ids_t,
    wq_hbm, wkv_hbm, wo_hbm, cache_hbm, gu_hbm, dn_hbm,
    out,
    rows, acts, wgu, wdn, placed, made, back,
    toks, wq, wkv, wo, cache, raw_gu, raw_dn,
    gain_pad, own_gain, tok_pad, qbuf, kvb, scb, resid, hid, placer, comb_hi, comb_lo,
    mine_f, mine_b, sib_b, chip_b, recv_b, table, small, small_t, posb, router_pad, scale_out, scale_in,
    wsem, lsem, d_send, d_recv, r_send, r_recv, x_send, x_recv,
    o_send, o_recv, a_send, a_recv, s_send, s_recv,
):
    dp = lax.axis_index("dp")
    tp = lax.axis_index("tp")
    z, y = lax.div(dp, NY), lax.rem(dp, NY)
    xx, core = lax.div(tp, 2), lax.rem(tp, 2)
    right = lax.rem(xx + 1, NX) * 2 + core
    left = lax.rem(xx + NX - 1, NX) * 2 + core
    across = lax.rem(xx + 2, NX) * 2 + core
    sib = xx * 2 + (1 - core)

    def flip(t):
        return t + 1 - 2 * core

    def cols(t):
        return pl.ds(pl.multiple_of(t * PAD, PAD), PAD)

    barrier = pltpu.get_barrier_semaphore()

    def greet(i, c):
        pl.semaphore_signal(
            barrier, inc=1, device_id=(lax.rem(dp + i, NZ * NY), tp), device_id_type=MESH
        )
        return c

    def greet_tp(i, c):
        pl.semaphore_signal(
            barrier, inc=1, device_id=(dp, lax.rem(tp + i, NTP)), device_id_type=MESH
        )
        return c

    lax.fori_loop(1, NTP, greet_tp, 0)
    lax.fori_loop(1, NZ * NY, greet, 0)

    get_q = [
        pltpu.make_async_copy(
            wq_hbm.at[pl.ds(b * COL, COL), :], wq.at[pl.ds(b * PAD, COL), :], wsem.at[b]
        )
        for b in range(NTP)
    ]
    get_kv = [
        pltpu.make_async_copy(
            wkv_hbm.at[pl.ds(b * COL, COL), :], wkv.at[pl.ds(b * PAD, COL), :], wsem.at[8 + b]
        )
        for b in range(NTP)
    ]
    get_o = [
        pltpu.make_async_copy(
            wo_hbm.at[pl.ds(b * COL, COL), :], wo.at[pl.ds(b * PAD, COL), :], wsem.at[16 + b]
        )
        for b in range(NTP)
    ]
    get_cache = pltpu.make_async_copy(cache_hbm, cache, wsem.at[24])
    get_gu = [
        pltpu.make_async_copy(gu_hbm.at[u], raw_gu.at[pl.ds(u * PAD, COL), :], wsem.at[25 + u])
        for u in range(2)
    ]
    get_dn = pltpu.make_async_copy(dn_hbm, raw_dn.at[pl.ds(0, COL), :], wsem.at[27])
    for group in (get_q, get_kv, [get_cache], get_o, get_gu, [get_dn]):
        for get in group:
            get.start()

    tok_pad[...] = jnp.zeros((TOK, PAD), F32)
    tok_pad[:, :COL] = tokens[...].astype(F32)
    toks[0, :, cols(tp)] = tok_pad[...].astype(BF)

    def xcopy(buf, ph, kind, j, part, col, dest):
        ref = buf.at[j, part, cols(col)]
        return pltpu.make_async_remote_copy(
            src_ref=ref,
            dst_ref=ref,
            send_sem=x_send.at[ph, kind, j],
            recv_sem=x_recv.at[ph, kind, j],
            device_id=(dp, dest),
            device_id_type=MESH,
        )

    def parts_of(buf):
        n = buf.shape[1]
        return pl.ds(0, n), pl.ds(0, n // 2), pl.ds(n // 2, n // 2)

    def straight(ph, j):
        if ph == 2:
            return STRAIGHT_TOKENS
        return j < STRAIGHT_ROWS if ph == 0 else j >= NZ - STRAIGHT_ACTS

    def send_own(buf, ph, j):
        allr, top, bot = parts_of(buf)

        @pl.when(straight(ph, j))
        def _():
            xcopy(buf, ph, 3, j, allr, tp, across).start()

        xcopy(buf, ph, 0, j, allr, tp, right).start()
        xcopy(buf, ph, 1, j, allr, tp, left).start()
        xcopy(buf, ph, 2, j, allr, tp, sib).start()

    def send_on(buf, ph, j):
        allr, top, bot = parts_of(buf)
        relayed = jnp.logical_not(straight(ph, j))
        xcopy(buf, ph, 0, j, allr, left, right).wait_recv()

        @pl.when(relayed)
        def _():
            xcopy(buf, ph, 3, j, top, left, right).start()

        xcopy(buf, ph, 4, j, allr, left, sib).start()
        xcopy(buf, ph, 1, j, allr, right, left).wait_recv()

        @pl.when(relayed)
        def _():
            xcopy(buf, ph, 5, j, bot, right, left).start()

        xcopy(buf, ph, 6, j, allr, right, sib).start()

    def send_far(buf, ph, j):
        allr, top, bot = parts_of(buf)

        @pl.when(straight(ph, j))
        def _():
            xcopy(buf, ph, 3, j, allr, across, across).wait_recv()

        @pl.when(jnp.logical_not(straight(ph, j)))
        def _():
            xcopy(buf, ph, 3, j, top, across, right).wait_recv()
            xcopy(buf, ph, 5, j, bot, across, left).wait_recv()

        xcopy(buf, ph, 7, j, allr, across, sib).start()

    def all_in(buf, ph, j):
        allr, top, bot = parts_of(buf)
        xcopy(buf, ph, 2, j, allr, sib, sib).wait_recv()
        xcopy(buf, ph, 4, j, allr, flip(left), sib).wait_recv()
        xcopy(buf, ph, 6, j, allr, flip(right), sib).wait_recv()
        xcopy(buf, ph, 7, j, allr, flip(across), sib).wait_recv()

    def all_sent(buf, ph, j):
        allr, top, bot = parts_of(buf)
        for kind in (0, 1, 2, 4, 6, 7):
            xcopy(buf, ph, kind, j, allr, tp, right).wait_send()

        @pl.when(straight(ph, j))
        def _():
            xcopy(buf, ph, 3, j, allr, tp, across).wait_send()

        @pl.when(jnp.logical_not(straight(ph, j)))
        def _():
            xcopy(buf, ph, 3, j, top, left, right).wait_send()
            xcopy(buf, ph, 5, j, bot, right, left).wait_send()

    pl.semaphore_wait(barrier, NZ * NY - 1 + NTP - 1)
    send_own(toks, 2, 0)

    for b in range(NTP):
        gain_pad[:, b * PAD + 2 * LANES : (b + 1) * PAD] = jnp.zeros((1, LANES), F32)
        gain_pad[:, b * PAD : b * PAD + COL] = gains[0:1, b * COL : (b + 1) * COL]
        own = gains[1:2, b * COL : (b + 1) * COL]

        @pl.when(tp == b)
        def _():
            own_gain[...] = jnp.zeros((1, PAD), F32)
            own_gain[:, :COL] = own

    small[...] = jnp.zeros((8, LANES), F32)
    small[0:1, :TOK] = pos[...].astype(F32)
    pos_col = jnp.transpose(jnp.broadcast_to(small[0:1, :], (LANES, LANES)))[:TOK]
    lane = lax.broadcasted_iota(jnp.int32, (TOK, LANES), 1)
    inverse = jnp.exp(
        lax.rem(lane, HD // 2).astype(F32) * (-2.0 / HD * math.log(rope_base))
    )
    angles = pos_col * inverse
    first = lax.rem(lane, HD) < HD // 2
    table[0] = jnp.cos(angles)
    sine = jnp.sin(angles)
    table[1] = jnp.where(first, -sine, sine)
    for g in range(8):
        posb[pl.ds(g, TOK, stride=8), :] = pos_col

    experts = NZ * NY
    e_iota = lax.broadcasted_iota(jnp.int32, (experts, TOK), 0)
    named = e_iota == ids_t[0:1, :]
    for k in range(1, ids_t.shape[0]):
        named = named | (e_iota == ids_t[k : k + 1, :])
    before = (
        lax.broadcasted_iota(jnp.int32, (TOK, TOK), 0)
        < lax.broadcasted_iota(jnp.int32, (TOK, TOK), 1)
    ).astype(F32)
    named_f = named.astype(F32)
    router_pad[...] = jnp.zeros((experts, PAD), BF)
    router_pad[:, :COL] = router_t[...]
    slot = jnp.dot(named_f, before, preferred_element_type=F32)
    slot = jnp.where(named, slot, -1.0)
    s_iota = lax.broadcasted_iota(jnp.int32, (SLOTS, TOK), 0).astype(F32)
    for e in range(experts):
        placer[e * SLOTS : (e + 1) * SLOTS, :] = (
            s_iota == slot[e : e + 1, :]
        ).astype(F32)

    send_on(toks, 2, 0)
    send_far(toks, 2, 0)
    for group, ref in ((get_q, wq), (get_kv, wkv), (get_o, wo)):
        for b, get in enumerate(group):
            get.wait()
            ref[b * PAD + COL : (b + 1) * PAD, :] = jnp.zeros((PAD - COL, ref.shape[1]), BF)
    all_in(toks, 2, 0)

    wide = toks[0].astype(F32)
    mean = jnp.sum(wide * wide, axis=1, keepdims=True) * (1.0 / FULL)
    normed = (wide * lax.rsqrt(mean + norm_eps) * gain_pad[...]).astype(BF)
    queries = jnp.dot(normed, wq[...], preferred_element_type=F32)
    fresh = jnp.dot(normed, wkv[...], preferred_element_type=F32)

    def turned(v):
        swapped = jnp.where(
            first, pltpu.roll(v, LANES - HD // 2, axis=1), pltpu.roll(v, HD // 2, axis=1)
        )
        return v * table[0] + swapped * table[1]

    entry = jnp.where(lane < HD, turned(fresh), fresh).astype(BF).astype(F32)
    qbuf[...] = jnp.zeros((SPAN, LANES), F32)
    kvb[...] = jnp.zeros((SPAN, LANES), F32)
    for g in range(HEADS):
        tile = g // 2
        if g % 2 == 0:
            rotated = turned(queries[:, tile * LANES : (tile + 1) * LANES]).astype(BF).astype(F32)
        head = rotated if g % 2 == 0 else pltpu.roll(rotated, HD, axis=1)
        qbuf[pl.ds(g, TOK, stride=8), :] = jnp.where(lane < HD, head * HD**-0.5, 0.0)
        kvb[pl.ds(g, TOK, stride=8), :] = entry
    get_cache.wait()

    sub = lax.broadcasted_iota(jnp.int32, (8, LANES), 0)
    sink = jnp.where(
        sub == 0,
        sinks[0],
        jnp.where(sub == 1, sinks[1], jnp.where(sub == 2, sinks[2], sinks[3])),
    )[:, :1]
    group = 24
    sink = jnp.concatenate([sink] * group, axis=0)
    slots = lax.broadcasted_iota(jnp.int32, (8 * group, LANES), 1)

    def attend(n, c):
        at = pl.ds(pl.multiple_of(n * 8 * group, 8 * group), 8 * group)
        asked = qbuf[at, :]
        entries = kvb[at, :]
        where_now = posb[at, :].astype(jnp.int32)
        newest = jnp.sum(asked * entries, axis=1, keepdims=True)
        raw = jnp.concatenate(
            [
                dot_nt(asked[8 * u : 8 * u + 8].astype(BF), cache[n * group + u])
                for u in range(group)
            ],
            axis=0,
        )
        current = slots == lax.rem(where_now, LANES)
        raw = jnp.where(current, newest, raw)
        raw = jnp.where(slots <= where_now, raw, -jnp.inf)
        peak = jnp.maximum(jnp.max(raw, axis=1, keepdims=True), sink)
        raised = jnp.exp(raw - peak)
        total = jnp.sum(raised, axis=1, keepdims=True) + jnp.exp(sink - peak)
        probs = (raised / total).astype(BF).astype(F32)
        newest_prob = (jnp.exp(newest - peak) / total).astype(BF).astype(F32)
        kept = jnp.where(current, 0.0, probs)
        mixed = jnp.concatenate(
            [
                jnp.dot(
                    kept[8 * u : 8 * u + 8].astype(BF),
                    cache[n * group + u],
                    preferred_element_type=F32,
                )
                for u in range(group)
            ],
            axis=0,
        )
        scb[at, :] = mixed + newest_prob * entries
        return c

    lax.fori_loop(0, TOK // group, attend, 0)
    tiles = []
    for tile in range(2):
        even = scb[pl.ds(2 * tile, TOK, stride=8), :]
        odd = scb[pl.ds(2 * tile + 1, TOK, stride=8), :]
        tiles.append(jnp.where(lane < HD, pltpu.roll(even, HD, axis=1), odd).astype(BF))
    attended = jnp.concatenate(tiles, axis=1)

    def out_block(owner):
        return dot_nt(attended, wo[cols(owner), :])

    for n in range(NX):
        mine_b[n] = out_block(2 * n + 1 - core).astype(BF)
    to_sib = pltpu.make_async_remote_copy(
        src_ref=mine_b,
        dst_ref=sib_b,
        send_sem=o_send.at[0],
        recv_sem=o_recv.at[0],
        device_id=(dp, sib),
        device_id_type=MESH,
    )
    to_sib.start()
    for n in range(NX):
        mine_f[n] = out_block(2 * n + core)
    to_sib.wait_recv()

    def to_chip(i):
        owner = lax.rem(xx + i, NX)
        return pltpu.make_async_remote_copy(
            src_ref=chip_b.at[owner],
            dst_ref=recv_b.at[i],
            send_sem=o_send.at[i],
            recv_sem=o_recv.at[i],
            device_id=(dp, owner * 2 + core),
            device_id_type=MESH,
        )

    for i in (2, 1, 3):
        owner = lax.rem(xx + i, NX)
        chip_b[owner] = (mine_f[owner] + sib_b[owner].astype(F32)).astype(BF)
        to_chip(i).start()
    total = tok_pad[...] + (mine_f[xx] + sib_b[xx].astype(F32))
    for get in get_gu:
        get.wait()
    raw_gu[COL:PAD, :] = jnp.zeros((PAD - COL, FULL), BF)
    raw_gu[PAD + COL : 2 * PAD, :] = jnp.zeros((PAD - COL, FULL), BF)
    spread_blocks(raw_gu, wgu, 2 * PAD, 48)
    get_dn.wait()
    raw_dn[COL:PAD, :] = jnp.zeros((PAD - COL, FULL), BF)
    spread_blocks(raw_dn, wdn, PAD, 48)
    for i in (1, 3, 2):
        to_chip(i).wait_recv()
    for i in (1, 2, 3):
        total = total + recv_b[i].astype(F32)
    resid[...] = total

    hid[...] = (total * own_gain[...]).astype(BF)

    def dispatch_copy(j, i):
        dest = lax.rem(z + NZ + NZ - z_offset(j), NZ) * NY + lax.rem(y + NY - i, NY)
        return pltpu.make_async_remote_copy(
            src_ref=placed.at[pl.ds(pl.multiple_of(dest * SLOTS, SLOTS), SLOTS), :],
            dst_ref=rows.at[j, pl.ds(pl.multiple_of(i * SLOTS, SLOTS), SLOTS), cols(tp)],
            send_sem=d_send.at[j * NY + i],
            recv_sem=d_recv.at[j * NY + i],
            device_id=(dest, tp),
            device_id_type=MESH,
        )

    own_in = pltpu.make_async_copy(
        placed.at[pl.ds(pl.multiple_of(dp * SLOTS, SLOTS), SLOTS), :],
        rows.at[OWN, pl.ds(0, SLOTS), cols(tp)],
        lsem.at[0],
    )

    def dispatch(j, c):
        zd = lax.rem(z + NZ + NZ - z_offset(j), NZ)
        part = pl.ds(pl.multiple_of(zd * CHUNK, CHUNK), CHUNK)
        placed[part, :] = jnp.dot(
            placer[part, :].astype(BF), hid[...], preferred_element_type=F32
        ).astype(BF)

        @pl.when(j == OWN)
        def _():
            own_in.start()

        @pl.when(j != OWN)
        def _():
            dispatch_copy(j, 0).start()

        for i in range(1, NY):
            dispatch_copy(j, i).start()
        return c

    lifted = total * own_gain[...]
    wide_rows = jnp.zeros((LANES - TOK, PAD), BF)
    logit_part = jnp.zeros((experts, LANES), F32)
    for piece in split3(lifted):
        logit_part = logit_part + dot_nt(router_pad[...], jnp.concatenate([piece, wide_rows], axis=0))
    square_part = jnp.zeros((8, LANES), F32)
    ones = jnp.ones((8, PAD), BF)
    for piece in split3(total * total):
        square_part = square_part + dot_nt(ones, jnp.concatenate([piece, wide_rows], axis=0))
    small_t[tp, 0:experts, :] = logit_part
    small_t[tp, experts : experts + 8, :] = square_part

    def share(i):
        return pltpu.make_async_remote_copy(
            src_ref=small_t.at[tp],
            dst_ref=small_t.at[tp],
            send_sem=a_send.at[i],
            recv_sem=a_recv.at[i],
            device_id=(dp, lax.rem(tp + i, NTP)),
            device_id_type=MESH,
        )

    for i in range(1, NTP):
        share(i).start()


    lax.fori_loop(0, AHEAD, dispatch, 0)

    def scale_copy(j, i):
        zd = lax.rem(z + NZ - z_offset(j), NZ)
        dest = zd * NY + lax.rem(y + NY - i, NY)
        return pltpu.make_async_remote_copy(
            src_ref=scale_out.at[zd],
            dst_ref=scale_in.at[j * NY + i],
            send_sem=s_send.at[j * NY + i],
            recv_sem=s_recv.at[j * NY + i],
            device_id=(dest, tp),
            device_id_type=MESH,
        )

    def scales_of(j):
        spot = lax.broadcasted_iota(jnp.int32, (1, LANES), 1)
        line = jnp.zeros((1, LANES), F32)
        for i in range(NY):

            @pl.when((j != OWN) | (i != 0))
            def _():
                scale_copy(j, i).wait_recv()

            there = pltpu.roll(
                jnp.broadcast_to(scale_in[j * NY + i], (8, LANES)),
                lax.rem(i + NY - y, NY) * SLOTS,
                axis=1,
            )[0:1]
            line = jnp.where(lax.div(spot, SLOTS) == i, there, line)
        return jnp.transpose(jnp.broadcast_to(line, (LANES, LANES)))[:, :1]

    def sums():
        summed = small_t[0]
        for n in range(1, NTP):
            summed = summed + small_t[n]
        scale_row = lax.rsqrt(summed[experts : experts + 1, :] * (1.0 / FULL) + norm_eps)
        return summed, scale_row

    def settle():
        for i in range(1, NTP):
            share(i).wait_recv()
        scale_row = sums()[1]
        hi, mid, low = split3(jnp.broadcast_to(scale_row[:, :TOK], (8, TOK)))
        which = lax.broadcasted_iota(jnp.int32, (8, TOK), 0)
        stacked = jnp.where(
            which == 0,
            hi.astype(F32),
            jnp.where(which == 1, mid.astype(F32), jnp.where(which == 2, low.astype(F32), 0.0)),
        ).astype(BF)
        for n in range(NZ):
            at = slice(n * CHUNK, (n + 1) * CHUNK)
            spots = placer[at, :].astype(BF)
            scale_out[n] = jnp.sum(dot_nt(stacked, spots), axis=0, keepdims=True)
        scale_in[OWN * NY] = scale_out[z]

        def send_scale(n, c):
            j, i = lax.div(n, NY), lax.rem(n, NY)

            @pl.when(n != OWN * NY)
            def _():
                scale_copy(j, i).start()

            return c

        lax.fori_loop(0, NZ * NY, send_scale, 0)

    def combine_weights():
        summed, scale_row = sums()
        logits = summed[0:experts, :TOK] * scale_row[:, :TOK]
        lifted_logits = jnp.where(named, jnp.exp(logits), 0.0)
        weights = lifted_logits / jnp.sum(lifted_logits, axis=0, keepdims=True)
        for e in range(experts):
            at = slice(e * SLOTS, (e + 1) * SLOTS)
            placer[at, :] = placer[at, :] * weights[e : e + 1, :]
        for n in range(NZ):
            at = slice(n * CHUNK, (n + 1) * CHUNK)
            piece = jnp.transpose(placer[at, :])
            hi = piece.astype(BF)
            comb_hi[:, at] = hi
            comb_lo[:, at] = (piece - hi.astype(F32)).astype(BF)

    def back_copy(j, i):
        home = lax.rem(z + z_offset(j), NZ) * NY + lax.rem(y + i, NY)
        return pltpu.make_async_remote_copy(
            src_ref=made.at[j, pl.ds(pl.multiple_of(i * SLOTS, SLOTS), SLOTS), :],
            dst_ref=back.at[pl.ds(pl.multiple_of(dp * SLOTS, SLOTS), SLOTS), :],
            send_sem=r_send.at[j * NY + i],
            recv_sem=r_recv.at[dp],
            device_id=(home, tp),
            device_id_type=MESH,
        )

    own_back = pltpu.make_async_copy(
        made.at[OWN, pl.ds(0, SLOTS), :],
        back.at[pl.ds(pl.multiple_of(dp * SLOTS, SLOTS), SLOTS), :],
        lsem.at[1],
    )

    def step(t, c):
        @pl.when((t >= 2) & (t < NZ + 2))
        def _():
            send_far(rows, 0, t - 2)

        @pl.when(t < NZ)
        def _():
            @pl.when(t == OWN)
            def _():
                own_in.wait()

            @pl.when(t != OWN)
            def _():
                dispatch_copy(t, 0).wait_recv()

            for i in range(1, NY):
                dispatch_copy(t, i).wait_recv()
            send_own(rows, 0, t)

        @pl.when(t == 0)
        def _():
            settle()

        @pl.when((t >= 1) & (t < NZ + 1))
        def _():
            send_on(rows, 0, t - 1)

        @pl.when(t < NZ - AHEAD)
        def _():
            dispatch(t + AHEAD, 0)

        @pl.when((t >= 2) & (t < NZ + 2))
        def _():
            j = t - 2
            scales = scales_of(j)
            all_in(rows, 0, j)
            mixed = dot_nt(rows[j], wgu[...]) * scales
            gate = mixed[:, :PAD]
            up = mixed[:, PAD:]
            act = gate * jax.nn.sigmoid(glu_alpha * gate) * (up + 1.0)
            acts[j, :, cols(tp)] = act.astype(BF)
            send_own(acts, 1, j)

        @pl.when(t >= 4)
        def _():
            send_far(acts, 1, t - 4)

        @pl.when((t >= 3) & (t < NZ + 3))
        def _():
            send_on(acts, 1, t - 3)

        @pl.when(t == NZ - AHEAD + 1)
        def _():
            combine_weights()

        @pl.when(t >= 4)
        def _():
            j = t - 4
            all_in(acts, 1, j)
            made[j] = dot_nt(acts[j], wdn[...]).astype(BF)

            @pl.when(j == OWN)
            def _():
                own_back.start()

            @pl.when(j != OWN)
            def _():
                back_copy(j, 0).start()

            for i in range(1, NY):
                back_copy(j, i).start()

        return c

    lax.fori_loop(0, NZ + 4, step, 0)

    def await_back(i, c):
        peer = lax.rem(dp + i, NZ * NY)
        pltpu.make_async_remote_copy(
            src_ref=made.at[0, pl.ds(0, SLOTS), :],
            dst_ref=back.at[pl.ds(pl.multiple_of(peer * SLOTS, SLOTS), SLOTS), :],
            send_sem=r_send.at[1],
            recv_sem=r_recv.at[peer],
            device_id=(peer, tp),
            device_id_type=MESH,
        ).wait_recv()
        return c

    own_back.wait()
    lax.fori_loop(1, NZ * NY, await_back, 0)
    got = back[...]
    answer = (
        resid[...]
        + jnp.dot(comb_hi[...], got, preferred_element_type=F32)
        + jnp.dot(comb_lo[...], got, preferred_element_type=F32)
    )
    out[...] = answer[:, :COL]

    to_sib.wait_send()
    for i in range(1, NX):
        to_chip(i).wait_send()
    for i in range(1, NTP):
        share(i).wait_send()
    all_sent(toks, 2, 0)

    def sent(n, c):
        @pl.when(n != OWN * NY)
        def _():
            j, i = lax.div(n, NY), lax.rem(n, NY)
            dispatch_copy(j, i).wait_send()
            back_copy(j, i).wait_send()
            scale_copy(j, i).wait_send()

        return c

    lax.fori_loop(0, NZ * NY, sent, 0)

    def sent_x(j, c):
        all_sent(rows, 0, j)
        all_sent(acts, 1, j)
        return c

    lax.fori_loop(0, NZ, sent_x, 0)


def on_device(
    tokens,
    attn_gain,
    w_query,
    w_keyvalue,
    attn_sinks,
    w_out,
    window_cache,
    positions,
    moe_gain,
    router,
    gate_up,
    w_down,
    expert_ids,
):
    vmem = pl.BlockSpec(memory_space=pltpu.VMEM)
    smem = pl.BlockSpec(memory_space=pltpu.SMEM)
    hbm = pl.BlockSpec(memory_space=pl.ANY)
    dma = pltpu.SemaphoreType.DMA
    vm = pltpu.VMEM
    return pl.pallas_call(
        layer_body,
        out_shape=jax.ShapeDtypeStruct(tokens.shape, F32),
        in_specs=[vmem, vmem, smem, vmem, vmem, vmem] + [hbm] * 6,
        out_specs=vmem,
        scratch_shapes=[
            vm((NZ, CHUNK, WIDE), BF),
            vm((NZ, CHUNK, WIDE), BF),
            vm((2 * PAD, WIDE), BF),
            vm((PAD, WIDE), BF),
            vm((NZ * CHUNK, PAD), BF),
            vm((NZ, CHUNK, PAD), BF),
            vm((NZ * CHUNK, PAD), BF),
            vm((1, TOK, WIDE), BF),
            vm((WIDE, HEADS * HD), BF),
            vm((WIDE, 2 * HD), BF),
            vm((WIDE, HEADS * HD), BF),
            vm((TOK, LANES, 2 * HD), BF),
            vm((2 * PAD, FULL), BF),
            vm((PAD, FULL), BF),
            vm((1, WIDE), F32),
            vm((1, PAD), F32),
            vm((TOK, PAD), F32),
            vm((SPAN, LANES), F32),
            vm((SPAN, LANES), F32),
            vm((SPAN, LANES), F32),
            vm((TOK, PAD), F32),
            vm((TOK, PAD), BF),
            vm((NZ * CHUNK, TOK), F32),
            vm((TOK, NZ * CHUNK), BF),
            vm((TOK, NZ * CHUNK), BF),
            vm((NX, TOK, PAD), F32),
            vm((NX, TOK, PAD), BF),
            vm((NX, TOK, PAD), BF),
            vm((NX, TOK, PAD), BF),
            vm((NX, TOK, PAD), BF),
            vm((2, TOK, LANES), F32),
            vm((8, LANES), F32),
            vm((NTP, 40, LANES), F32),
            vm((SPAN, LANES), F32),
            vm((NZ * NY, PAD), BF),
            vm((NZ, 1, LANES), F32),
            vm((NZ * NY, 1, LANES), F32),
            dma((28,)),
            dma((2,)),
            dma((NZ * NY,)),
            dma((NZ * NY,)),
            dma((NZ * NY,)),
            dma((NZ * NY,)),
            dma((3, 8, NZ)),
            dma((3, 8, NZ)),
            dma((NX,)),
            dma((NX,)),
            dma((NTP,)),
            dma((NTP,)),
            dma((NZ * NY,)),
            dma((NZ * NY,)),
        ],
        compiler_params=pltpu.CompilerParams(
            collective_id=0, has_side_effects=True, vmem_limit_bytes=60 * 1024 * 1024
        ),
        name="layer",
    )(
        tokens,
        jnp.stack([attn_gain, moe_gain]),
        attn_sinks,
        positions[None, :],
        jnp.transpose(router),
        jnp.transpose(expert_ids),
        w_query,
        w_keyvalue.reshape(FULL, 2 * HD),
        jnp.transpose(w_out),
        window_cache.reshape(TOK, LANES, 2 * HD),
        jnp.transpose(gate_up[0], (1, 2, 0)),
        jnp.transpose(w_down[0]),
    )


def solution(mesh):
    in_specs = (
        P("dp", "tp"),
        P(),
        P(None, "tp"),
        P(None, "tp", None),
        P("tp"),
        P("tp", None),
        P("dp", "tp", None, None),
        P("dp"),
        P(),
        P("tp", None),
        P("dp", None, None, "tp"),
        P("dp", None, "tp"),
        P("dp", None),
    )
    out_specs = P("dp", "tp")
    return jax.shard_map(
        on_device, mesh=mesh, in_specs=in_specs, out_specs=out_specs, check_vma=False
    )
```

```python
import math

import jax
import jax.numpy as jnp
from jax import lax
from jax.experimental import pallas as pl
from jax.experimental.pallas import tpu as pltpu
from jax.sharding import PartitionSpec as P

norm_eps = 1e-05
rope_base = 150000.0
glu_alpha = 1.702

COL = 360
PAD = 384
FULL = 2880
NZ = 8
NY = 4
NX = 4
NTP = 2 * NX
SLOTS = 32
GROUP = NY * SLOTS
PAIR = 4
CHUNK = PAIR * SLOTS
PARTS = NY // PAIR
NC = NZ * PARTS
WIDE = NTP * PAD
TOK = 96
HEADS = 4
HD = 64
LANES = 128
SPAN = 8 * TOK
MESH = pl.DeviceIdType.MESH
NT = (((1,), (1,)), ((), ()))
F32 = jnp.float32
BF = jnp.bfloat16


ORDER = (0, 1, 2, 4, 5, 3, 6, 7)
OWN = ORDER.index(0)
SETTLE = 1
AHEAD = 3
STRAIGHT_ROWS = 1
STRAIGHT_ACTS = 0
ON, FAR, GATE, ACT_ON, ACT_FAR, DOWN = 1, 2, 3, 4, 5, 6
STRAIGHT_TOKENS = True


def z_offset(j):
    offset = 0
    for n, value in enumerate(ORDER):
        offset = jnp.where(j == n, value, offset)
    return offset


def dot_nt(a, b):
    return lax.dot_general(a, b, NT, preferred_element_type=F32)


def split3(v):
    hi = v.astype(BF)
    rest = v - hi.astype(F32)
    mid = rest.astype(BF)
    low = (rest - mid.astype(F32)).astype(BF)
    return hi, mid, low


def spread_blocks(src, dst, rows, row_step):
    def part(n, c):
        at = pl.ds(pl.multiple_of(n * row_step, row_step), row_step)
        for b in range(NTP):
            low = b * COL // LANES * LANES
            off = b * COL - low
            high = min(low + 4 * LANES, FULL)
            piece = src[at, low:high]
            dst[at, b * PAD + 2 * LANES : (b + 1) * PAD] = jnp.zeros((row_step, LANES), dst.dtype)
            dst[at, b * PAD : b * PAD + COL] = piece[:, off : off + COL]
        return c

    lax.fori_loop(0, rows // row_step, part, 0)


def layer_body(
    tokens, gains, sinks, pos, router_t, ids_t,
    wq_hbm, wkv_hbm, wo_hbm, cache_hbm, gu_hbm, dn_hbm,
    out,
    rows, acts, wgu, wdn, placed, made, back,
    toks, wq, wkv, wo, cache, raw_gu, raw_dn,
    gain_pad, own_gain, tok_pad, qbuf, kvb, scb, resid, hid, placer, comb_hi, comb_lo,
    mine_f, mine_b, sib_b, chip_b, recv_b, table, small, small_t, posb, router_pad, scale_out, scale_in,
    wsem, lsem, d_send, d_recv, r_send, r_recv, x_send, x_recv,
    o_send, o_recv, a_send, a_recv, s_send, s_recv,
):
    dp = lax.axis_index("dp")
    tp = lax.axis_index("tp")
    z, y = lax.div(dp, NY), lax.rem(dp, NY)
    xx, core = lax.div(tp, 2), lax.rem(tp, 2)
    right = lax.rem(xx + 1, NX) * 2 + core
    left = lax.rem(xx + NX - 1, NX) * 2 + core
    across = lax.rem(xx + 2, NX) * 2 + core
    sib = xx * 2 + (1 - core)

    def flip(t):
        return t + 1 - 2 * core

    def cols(t):
        return pl.ds(pl.multiple_of(t * PAD, PAD), PAD)

    barrier = pltpu.get_barrier_semaphore()

    def greet(i, c):
        pl.semaphore_signal(
            barrier, inc=1, device_id=(lax.rem(dp + i, NZ * NY), tp), device_id_type=MESH
        )
        return c

    def greet_tp(i, c):
        pl.semaphore_signal(
            barrier, inc=1, device_id=(dp, lax.rem(tp + i, NTP)), device_id_type=MESH
        )
        return c

    lax.fori_loop(1, NTP, greet_tp, 0)
    lax.fori_loop(1, NZ * NY, greet, 0)

    get_q = [
        pltpu.make_async_copy(
            wq_hbm.at[pl.ds(b * COL, COL), :], wq.at[pl.ds(b * PAD, COL), :], wsem.at[b]
        )
        for b in range(NTP)
    ]
    get_kv = [
        pltpu.make_async_copy(
            wkv_hbm.at[pl.ds(b * COL, COL), :], wkv.at[pl.ds(b * PAD, COL), :], wsem.at[8 + b]
        )
        for b in range(NTP)
    ]
    get_o = [
        pltpu.make_async_copy(
            wo_hbm.at[pl.ds(b * COL, COL), :], wo.at[pl.ds(b * PAD, COL), :], wsem.at[16 + b]
        )
        for b in range(NTP)
    ]
    get_cache = pltpu.make_async_copy(cache_hbm, cache, wsem.at[24])
    get_gu = [
        pltpu.make_async_copy(gu_hbm.at[u], raw_gu.at[pl.ds(u * PAD, COL), :], wsem.at[25 + u])
        for u in range(2)
    ]
    get_dn = pltpu.make_async_copy(dn_hbm, raw_dn.at[pl.ds(0, COL), :], wsem.at[27])
    for group in (get_q, get_kv, [get_cache], get_o, get_gu, [get_dn]):
        for get in group:
            get.start()

    tok_pad[...] = jnp.zeros((TOK, PAD), F32)
    tok_pad[:, :COL] = tokens[...].astype(F32)
    toks[0, :, cols(tp)] = tok_pad[...].astype(BF)

    def xcopy(buf, ph, kind, j, part, col, dest):
        ref = buf.at[j, part, cols(col)]
        return pltpu.make_async_remote_copy(
            src_ref=ref,
            dst_ref=ref,
            send_sem=x_send.at[ph, kind, j],
            recv_sem=x_recv.at[ph, kind, j],
            device_id=(dp, dest),
            device_id_type=MESH,
        )

    def parts_of(buf):
        n = buf.shape[1]
        return pl.ds(0, n), pl.ds(0, n // 2), pl.ds(n // 2, n // 2)

    def straight(ph, j):
        if ph == 2:
            return STRAIGHT_TOKENS
        return j < STRAIGHT_ROWS if ph == 0 else j >= NC - STRAIGHT_ACTS

    def send_own(buf, ph, j):
        allr, top, bot = parts_of(buf)

        @pl.when(straight(ph, j))
        def _():
            xcopy(buf, ph, 3, j, allr, tp, across).start()

        xcopy(buf, ph, 0, j, allr, tp, right).start()
        xcopy(buf, ph, 1, j, allr, tp, left).start()
        xcopy(buf, ph, 2, j, allr, tp, sib).start()

    def send_on(buf, ph, j):
        allr, top, bot = parts_of(buf)
        relayed = jnp.logical_not(straight(ph, j))
        xcopy(buf, ph, 0, j, allr, left, right).wait_recv()

        @pl.when(relayed)
        def _():
            xcopy(buf, ph, 3, j, top, left, right).start()

        xcopy(buf, ph, 4, j, allr, left, sib).start()
        xcopy(buf, ph, 1, j, allr, right, left).wait_recv()

        @pl.when(relayed)
        def _():
            xcopy(buf, ph, 5, j, bot, right, left).start()

        xcopy(buf, ph, 6, j, allr, right, sib).start()

    def send_far(buf, ph, j):
        allr, top, bot = parts_of(buf)

        @pl.when(straight(ph, j))
        def _():
            xcopy(buf, ph, 3, j, allr, across, across).wait_recv()

        @pl.when(jnp.logical_not(straight(ph, j)))
        def _():
            xcopy(buf, ph, 3, j, top, across, right).wait_recv()
            xcopy(buf, ph, 5, j, bot, across, left).wait_recv()

        xcopy(buf, ph, 7, j, allr, across, sib).start()

    def all_in(buf, ph, j):
        allr, top, bot = parts_of(buf)
        xcopy(buf, ph, 2, j, allr, sib, sib).wait_recv()
        xcopy(buf, ph, 4, j, allr, flip(left), sib).wait_recv()
        xcopy(buf, ph, 6, j, allr, flip(right), sib).wait_recv()
        xcopy(buf, ph, 7, j, allr, flip(across), sib).wait_recv()

    def all_sent(buf, ph, j):
        allr, top, bot = parts_of(buf)
        for kind in (0, 1, 2, 4, 6, 7):
            xcopy(buf, ph, kind, j, allr, tp, right).wait_send()

        @pl.when(straight(ph, j))
        def _():
            xcopy(buf, ph, 3, j, allr, tp, across).wait_send()

        @pl.when(jnp.logical_not(straight(ph, j)))
        def _():
            xcopy(buf, ph, 3, j, top, left, right).wait_send()
            xcopy(buf, ph, 5, j, bot, right, left).wait_send()

    pl.semaphore_wait(barrier, NZ * NY - 1 + NTP - 1)
    send_own(toks, 2, 0)

    for b in range(NTP):
        gain_pad[:, b * PAD + 2 * LANES : (b + 1) * PAD] = jnp.zeros((1, LANES), F32)
        gain_pad[:, b * PAD : b * PAD + COL] = gains[0:1, b * COL : (b + 1) * COL]
        own = gains[1:2, b * COL : (b + 1) * COL]

        @pl.when(tp == b)
        def _():
            own_gain[...] = jnp.zeros((1, PAD), F32)
            own_gain[:, :COL] = own

    small[...] = jnp.zeros((8, LANES), F32)
    small[0:1, :TOK] = pos[...].astype(F32)
    pos_col = jnp.transpose(jnp.broadcast_to(small[0:1, :], (LANES, LANES)))[:TOK]
    lane = lax.broadcasted_iota(jnp.int32, (TOK, LANES), 1)
    inverse = jnp.exp(
        lax.rem(lane, HD // 2).astype(F32) * (-2.0 / HD * math.log(rope_base))
    )
    angles = pos_col * inverse
    first = lax.rem(lane, HD) < HD // 2
    table[0] = jnp.cos(angles)
    sine = jnp.sin(angles)
    table[1] = jnp.where(first, -sine, sine)
    for g in range(8):
        posb[pl.ds(g, TOK, stride=8), :] = pos_col

    experts = NZ * NY
    e_iota = lax.broadcasted_iota(jnp.int32, (experts, TOK), 0)
    named = e_iota == ids_t[0:1, :]
    for k in range(1, ids_t.shape[0]):
        named = named | (e_iota == ids_t[k : k + 1, :])
    before = (
        lax.broadcasted_iota(jnp.int32, (TOK, TOK), 0)
        < lax.broadcasted_iota(jnp.int32, (TOK, TOK), 1)
    ).astype(F32)
    named_f = named.astype(F32)
    router_pad[...] = jnp.zeros((experts, PAD), BF)
    router_pad[:, :COL] = router_t[...]
    slot = jnp.dot(named_f, before, preferred_element_type=F32)
    slot = jnp.where(named, slot, -1.0)
    s_iota = lax.broadcasted_iota(jnp.int32, (SLOTS, TOK), 0).astype(F32)
    for e in range(experts):
        placer[e * SLOTS : (e + 1) * SLOTS, :] = (
            s_iota == slot[e : e + 1, :]
        ).astype(F32)

    send_on(toks, 2, 0)
    send_far(toks, 2, 0)
    for group, ref in ((get_q, wq), (get_kv, wkv), (get_o, wo)):
        for b, get in enumerate(group):
            get.wait()
            ref[b * PAD + COL : (b + 1) * PAD, :] = jnp.zeros((PAD - COL, ref.shape[1]), BF)
    all_in(toks, 2, 0)

    wide = toks[0].astype(F32)
    mean = jnp.sum(wide * wide, axis=1, keepdims=True) * (1.0 / FULL)
    normed = (wide * lax.rsqrt(mean + norm_eps) * gain_pad[...]).astype(BF)
    queries = jnp.dot(normed, wq[...], preferred_element_type=F32)
    fresh = jnp.dot(normed, wkv[...], preferred_element_type=F32)

    def turned(v):
        swapped = jnp.where(
            first, pltpu.roll(v, LANES - HD // 2, axis=1), pltpu.roll(v, HD // 2, axis=1)
        )
        return v * table[0] + swapped * table[1]

    entry = jnp.where(lane < HD, turned(fresh), fresh).astype(BF).astype(F32)
    qbuf[...] = jnp.zeros((SPAN, LANES), F32)
    kvb[...] = jnp.zeros((SPAN, LANES), F32)
    for g in range(HEADS):
        tile = g // 2
        if g % 2 == 0:
            rotated = turned(queries[:, tile * LANES : (tile + 1) * LANES]).astype(BF).astype(F32)
        head = rotated if g % 2 == 0 else pltpu.roll(rotated, HD, axis=1)
        qbuf[pl.ds(g, TOK, stride=8), :] = jnp.where(lane < HD, head * HD**-0.5, 0.0)
        kvb[pl.ds(g, TOK, stride=8), :] = entry
    get_cache.wait()

    sub = lax.broadcasted_iota(jnp.int32, (8, LANES), 0)
    sink = jnp.where(
        sub == 0,
        sinks[0],
        jnp.where(sub == 1, sinks[1], jnp.where(sub == 2, sinks[2], sinks[3])),
    )[:, :1]
    group = 48
    sink = jnp.concatenate([sink] * group, axis=0)
    slots = lax.broadcasted_iota(jnp.int32, (8 * group, LANES), 1)

    def attend(n, c):
        at = pl.ds(pl.multiple_of(n * 8 * group, 8 * group), 8 * group)
        asked = qbuf[at, :]
        entries = kvb[at, :]
        where_now = posb[at, :].astype(jnp.int32)
        newest = jnp.sum(asked * entries, axis=1, keepdims=True)
        raw = jnp.concatenate(
            [
                dot_nt(asked[8 * u : 8 * u + 8].astype(BF), cache[n * group + u])
                for u in range(group)
            ],
            axis=0,
        )
        current = slots == lax.rem(where_now, LANES)
        raw = jnp.where(current, newest, raw)
        raw = jnp.where(slots <= where_now, raw, -jnp.inf)
        peak = jnp.maximum(jnp.max(raw, axis=1, keepdims=True), sink)
        raised = jnp.exp(raw - peak)
        total = jnp.sum(raised, axis=1, keepdims=True) + jnp.exp(sink - peak)
        probs = (raised / total).astype(BF).astype(F32)
        newest_prob = (jnp.exp(newest - peak) / total).astype(BF).astype(F32)
        kept = jnp.where(current, 0.0, probs)
        mixed = jnp.concatenate(
            [
                jnp.dot(
                    kept[8 * u : 8 * u + 8].astype(BF),
                    cache[n * group + u],
                    preferred_element_type=F32,
                )
                for u in range(group)
            ],
            axis=0,
        )
        scb[at, :] = mixed + newest_prob * entries
        return c

    lax.fori_loop(0, TOK // group, attend, 0)
    tiles = []
    for tile in range(2):
        even = scb[pl.ds(2 * tile, TOK, stride=8), :]
        odd = scb[pl.ds(2 * tile + 1, TOK, stride=8), :]
        tiles.append(jnp.where(lane < HD, pltpu.roll(even, HD, axis=1), odd).astype(BF))
    attended = jnp.concatenate(tiles, axis=1)

    def out_block(owner):
        return dot_nt(attended, wo[cols(owner), :])

    for n in range(NX):
        mine_b[n] = out_block(2 * n + 1 - core).astype(BF)
    to_sib = pltpu.make_async_remote_copy(
        src_ref=mine_b,
        dst_ref=sib_b,
        send_sem=o_send.at[0],
        recv_sem=o_recv.at[0],
        device_id=(dp, sib),
        device_id_type=MESH,
    )
    to_sib.start()
    for n in range(NX):
        mine_f[n] = out_block(2 * n + core)
    to_sib.wait_recv()

    def to_chip(i):
        owner = lax.rem(xx + i, NX)
        return pltpu.make_async_remote_copy(
            src_ref=chip_b.at[owner],
            dst_ref=recv_b.at[i],
            send_sem=o_send.at[i],
            recv_sem=o_recv.at[i],
            device_id=(dp, owner * 2 + core),
            device_id_type=MESH,
        )

    for i in (2, 1, 3):
        owner = lax.rem(xx + i, NX)
        chip_b[owner] = (mine_f[owner] + sib_b[owner].astype(F32)).astype(BF)
        to_chip(i).start()
    total = tok_pad[...] + (mine_f[xx] + sib_b[xx].astype(F32))
    for get in get_gu:
        get.wait()
    raw_gu[COL:PAD, :] = jnp.zeros((PAD - COL, FULL), BF)
    raw_gu[PAD + COL : 2 * PAD, :] = jnp.zeros((PAD - COL, FULL), BF)
    spread_blocks(raw_gu, wgu, 2 * PAD, 48)
    get_dn.wait()
    raw_dn[COL:PAD, :] = jnp.zeros((PAD - COL, FULL), BF)
    spread_blocks(raw_dn, wdn, PAD, 48)
    for i in (1, 3, 2):
        to_chip(i).wait_recv()
    for i in (1, 2, 3):
        total = total + recv_b[i].astype(F32)
    resid[...] = total

    hid[...] = (total * own_gain[...]).astype(BF)

    def within(i):
        return pl.ds(pl.multiple_of(lax.rem(i, PAIR) * SLOTS, SLOTS), SLOTS)

    def dispatch_copy(j, i):
        dest = lax.rem(z + NZ + NZ - z_offset(j), NZ) * NY + lax.rem(y + NY - i, NY)
        return pltpu.make_async_remote_copy(
            src_ref=placed.at[pl.ds(pl.multiple_of(dest * SLOTS, SLOTS), SLOTS), :],
            dst_ref=rows.at[j * PARTS + lax.div(i, PAIR), within(i), cols(tp)],
            send_sem=d_send.at[j * NY + i],
            recv_sem=d_recv.at[j * NY + i],
            device_id=(dest, tp),
            device_id_type=MESH,
        )

    own_in = pltpu.make_async_copy(
        placed.at[pl.ds(pl.multiple_of(dp * SLOTS, SLOTS), SLOTS), :],
        rows.at[OWN * PARTS, pl.ds(0, SLOTS), cols(tp)],
        lsem.at[0],
    )

    def dispatch(j, c):
        zd = lax.rem(z + NZ + NZ - z_offset(j), NZ)
        part = pl.ds(pl.multiple_of(zd * GROUP, GROUP), GROUP)
        placed[part, :] = jnp.dot(
            placer[part, :].astype(BF), hid[...], preferred_element_type=F32
        ).astype(BF)

        @pl.when(j == OWN)
        def _():
            own_in.start()

        @pl.when(j != OWN)
        def _():
            dispatch_copy(j, 0).start()

        for i in range(1, NY):
            dispatch_copy(j, i).start()
        return c

    lifted = total * own_gain[...]
    wide_rows = jnp.zeros((LANES - TOK, PAD), BF)
    logit_part = jnp.zeros((experts, LANES), F32)
    for piece in split3(lifted):
        logit_part = logit_part + dot_nt(router_pad[...], jnp.concatenate([piece, wide_rows], axis=0))
    square_part = jnp.zeros((8, LANES), F32)
    ones = jnp.ones((8, PAD), BF)
    for piece in split3(total * total):
        square_part = square_part + dot_nt(ones, jnp.concatenate([piece, wide_rows], axis=0))
    small_t[tp, 0:experts, :] = logit_part
    small_t[tp, experts : experts + 8, :] = square_part

    def share(i):
        return pltpu.make_async_remote_copy(
            src_ref=small_t.at[tp],
            dst_ref=small_t.at[tp],
            send_sem=a_send.at[i],
            recv_sem=a_recv.at[i],
            device_id=(dp, lax.rem(tp + i, NTP)),
            device_id_type=MESH,
        )

    for i in range(1, NTP):
        share(i).start()


    lax.fori_loop(0, AHEAD, dispatch, 0)

    def scale_copy(j, i):
        zd = lax.rem(z + NZ - z_offset(j), NZ)
        dest = zd * NY + lax.rem(y + NY - i, NY)
        return pltpu.make_async_remote_copy(
            src_ref=scale_out.at[zd],
            dst_ref=scale_in.at[j * NY + i],
            send_sem=s_send.at[j * NY + i],
            recv_sem=s_recv.at[j * NY + i],
            device_id=(dest, tp),
            device_id_type=MESH,
        )

    def scales_of(c):
        spot = lax.broadcasted_iota(jnp.int32, (1, LANES), 1)
        line = jnp.zeros((1, LANES), F32)
        for k in range(PAIR):
            n = c * PAIR + k

            @pl.when(n != OWN * NY)
            def _():
                scale_copy(lax.div(n, NY), lax.rem(n, NY)).wait_recv()

            there = pltpu.roll(
                jnp.broadcast_to(scale_in[n], (8, LANES)),
                lax.rem(k + NY - y, NY) * SLOTS,
                axis=1,
            )[0:1]
            line = jnp.where(lax.div(spot, SLOTS) == k, there, line)
        return jnp.transpose(jnp.broadcast_to(line, (LANES, LANES)))[:CHUNK, :1]

    def sums():
        summed = small_t[0]
        for n in range(1, NTP):
            summed = summed + small_t[n]
        scale_row = lax.rsqrt(summed[experts : experts + 1, :] * (1.0 / FULL) + norm_eps)
        return summed, scale_row

    def settle():
        for i in range(1, NTP):
            share(i).wait_recv()
        scale_row = sums()[1]
        hi, mid, low = split3(jnp.broadcast_to(scale_row[:, :TOK], (8, TOK)))
        which = lax.broadcasted_iota(jnp.int32, (8, TOK), 0)
        stacked = jnp.where(
            which == 0,
            hi.astype(F32),
            jnp.where(which == 1, mid.astype(F32), jnp.where(which == 2, low.astype(F32), 0.0)),
        ).astype(BF)
        for n in range(NZ):
            at = slice(n * GROUP, (n + 1) * GROUP)
            spots = placer[at, :].astype(BF)
            scale_out[n] = jnp.sum(dot_nt(stacked, spots), axis=0, keepdims=True)
        scale_in[OWN * NY] = scale_out[z]

        def send_scale(n, c):
            j, i = lax.div(n, NY), lax.rem(n, NY)

            @pl.when(n != OWN * NY)
            def _():
                scale_copy(j, i).start()

            return c

        lax.fori_loop(0, NZ * NY, send_scale, 0)

    def combine_weights():
        summed, scale_row = sums()
        logits = summed[0:experts, :TOK] * scale_row[:, :TOK]
        lifted_logits = jnp.where(named, jnp.exp(logits), 0.0)
        weights = lifted_logits / jnp.sum(lifted_logits, axis=0, keepdims=True)
        for e in range(experts):
            at = slice(e * SLOTS, (e + 1) * SLOTS)
            placer[at, :] = placer[at, :] * weights[e : e + 1, :]
        for n in range(NZ):
            at = slice(n * GROUP, (n + 1) * GROUP)
            piece = jnp.transpose(placer[at, :])
            hi = piece.astype(BF)
            comb_hi[:, at] = hi
            comb_lo[:, at] = (piece - hi.astype(F32)).astype(BF)

    def back_copy(j, i):
        home = lax.rem(z + z_offset(j), NZ) * NY + lax.rem(y + i, NY)
        return pltpu.make_async_remote_copy(
            src_ref=made.at[j * PARTS + lax.div(i, PAIR), within(i), :],
            dst_ref=back.at[pl.ds(pl.multiple_of(dp * SLOTS, SLOTS), SLOTS), :],
            send_sem=r_send.at[j * NY + i],
            recv_sem=r_recv.at[dp],
            device_id=(home, tp),
            device_id_type=MESH,
        )

    own_back = pltpu.make_async_copy(
        made.at[OWN * PARTS, pl.ds(0, SLOTS), :],
        back.at[pl.ds(pl.multiple_of(dp * SLOTS, SLOTS), SLOTS), :],
        lsem.at[1],
    )

    def step(t, c):
        @pl.when(t < NC)
        def _():
            for k in range(PAIR):
                n = t * PAIR + k

                @pl.when(n == OWN * NY)
                def _():
                    own_in.wait()

                @pl.when(n != OWN * NY)
                def _():
                    dispatch_copy(lax.div(n, NY), lax.rem(n, NY)).wait_recv()

            send_own(rows, 0, t)

        @pl.when(t == SETTLE)
        def _():
            settle()

        @pl.when((t >= ON) & (t < NC + ON))
        def _():
            send_on(rows, 0, t - ON)

        @pl.when((lax.rem(t, PARTS) == 0) & (t < (NZ - AHEAD) * PARTS))
        def _():
            dispatch(lax.div(t, PARTS) + AHEAD, 0)

        @pl.when((t >= GATE) & (t < NC + GATE))
        def _():
            j = t - GATE
            scales = scales_of(j)
            all_in(rows, 0, j)
            mixed = dot_nt(rows[j], wgu[...]) * scales
            gate = mixed[:, :PAD]
            up = mixed[:, PAD:]
            act = gate * jax.nn.sigmoid(glu_alpha * gate) * (up + 1.0)
            acts[j, :, cols(tp)] = act.astype(BF)
            send_own(acts, 1, j)

        @pl.when((t >= FAR) & (t < NC + FAR))
        def _():
            send_far(rows, 0, t - FAR)

        @pl.when((t >= ACT_ON) & (t < NC + ACT_ON))
        def _():
            send_on(acts, 1, t - ACT_ON)

        @pl.when(t == (NZ - AHEAD) * PARTS + 1)
        def _():
            combine_weights()

        @pl.when((t >= DOWN) & (t < NC + DOWN))
        def _():
            j = t - DOWN
            all_in(acts, 1, j)
            made[j] = dot_nt(acts[j], wdn[...]).astype(BF)
            for k in range(PAIR):
                n = j * PAIR + k

                @pl.when(n == OWN * NY)
                def _():
                    own_back.start()

                @pl.when(n != OWN * NY)
                def _():
                    back_copy(lax.div(n, NY), lax.rem(n, NY)).start()

        @pl.when((t >= ACT_FAR) & (t < NC + ACT_FAR))
        def _():
            send_far(acts, 1, t - ACT_FAR)

        return c

    lax.fori_loop(0, NC + DOWN, step, 0)

    to_sib.wait_send()
    for i in range(1, NX):
        to_chip(i).wait_send()
    for i in range(1, NTP):
        share(i).wait_send()
    all_sent(toks, 2, 0)

    def sent(n, c):
        @pl.when(n != OWN * NY)
        def _():
            j, i = lax.div(n, NY), lax.rem(n, NY)
            dispatch_copy(j, i).wait_send()
            back_copy(j, i).wait_send()
            scale_copy(j, i).wait_send()

        return c

    lax.fori_loop(0, NZ * NY, sent, 0)

    def sent_x(j, c):
        all_sent(rows, 0, j)
        all_sent(acts, 1, j)
        return c

    lax.fori_loop(0, NC, sent_x, 0)

    def await_back(i, c):
        peer = lax.rem(dp + i, NZ * NY)
        pltpu.make_async_remote_copy(
            src_ref=made.at[0, pl.ds(0, SLOTS), :],
            dst_ref=back.at[pl.ds(pl.multiple_of(peer * SLOTS, SLOTS), SLOTS), :],
            send_sem=r_send.at[1],
            recv_sem=r_recv.at[peer],
            device_id=(peer, tp),
            device_id_type=MESH,
        ).wait_recv()
        return c

    own_back.wait()
    lax.fori_loop(1, NZ * NY, await_back, 0)
    got = back[...]
    answer = (
        resid[...]
        + jnp.dot(comb_hi[...], got, preferred_element_type=F32)
        + jnp.dot(comb_lo[...], got, preferred_element_type=F32)
    )
    out[...] = answer[:, :COL]


def on_device(
    tokens,
    attn_gain,
    w_query,
    w_keyvalue,
    attn_sinks,
    w_out,
    window_cache,
    positions,
    moe_gain,
    router,
    gate_up,
    w_down,
    expert_ids,
):
    vmem = pl.BlockSpec(memory_space=pltpu.VMEM)
    smem = pl.BlockSpec(memory_space=pltpu.SMEM)
    hbm = pl.BlockSpec(memory_space=pl.ANY)
    dma = pltpu.SemaphoreType.DMA
    vm = pltpu.VMEM
    return pl.pallas_call(
        layer_body,
        out_shape=jax.ShapeDtypeStruct(tokens.shape, F32),
        in_specs=[vmem, vmem, smem, vmem, vmem, vmem] + [hbm] * 6,
        out_specs=vmem,
        scratch_shapes=[
            vm((NC, CHUNK, WIDE), BF),
            vm((NC, CHUNK, WIDE), BF),
            vm((2 * PAD, WIDE), BF),
            vm((PAD, WIDE), BF),
            vm((NZ * GROUP, PAD), BF),
            vm((NC, CHUNK, PAD), BF),
            vm((NZ * GROUP, PAD), BF),
            vm((1, TOK, WIDE), BF),
            vm((WIDE, HEADS * HD), BF),
            vm((WIDE, 2 * HD), BF),
            vm((WIDE, HEADS * HD), BF),
            vm((TOK, LANES, 2 * HD), BF),
            vm((2 * PAD, FULL), BF),
            vm((PAD, FULL), BF),
            vm((1, WIDE), F32),
            vm((1, PAD), F32),
            vm((TOK, PAD), F32),
            vm((SPAN, LANES), F32),
            vm((SPAN, LANES), F32),
            vm((SPAN, LANES), F32),
            vm((TOK, PAD), F32),
            vm((TOK, PAD), BF),
            vm((NZ * GROUP, TOK), F32),
            vm((TOK, NZ * GROUP), BF),
            vm((TOK, NZ * GROUP), BF),
            vm((NX, TOK, PAD), F32),
            vm((NX, TOK, PAD), BF),
            vm((NX, TOK, PAD), BF),
            vm((NX, TOK, PAD), BF),
            vm((NX, TOK, PAD), BF),
            vm((2, TOK, LANES), F32),
            vm((8, LANES), F32),
            vm((NTP, 40, LANES), F32),
            vm((SPAN, LANES), F32),
            vm((NZ * NY, PAD), BF),
            vm((NZ, 1, LANES), F32),
            vm((NZ * NY, 1, LANES), F32),
            dma((28,)),
            dma((2,)),
            dma((NZ * NY,)),
            dma((NZ * NY,)),
            dma((NZ * NY,)),
            dma((NZ * NY,)),
            dma((3, 8, NC)),
            dma((3, 8, NC)),
            dma((NX,)),
            dma((NX,)),
            dma((NTP,)),
            dma((NTP,)),
            dma((NZ * NY,)),
            dma((NZ * NY,)),
        ],
        compiler_params=pltpu.CompilerParams(
            collective_id=0, has_side_effects=True, vmem_limit_bytes=60 * 1024 * 1024
        ),
        name="layer",
    )(
        tokens,
        jnp.stack([attn_gain, moe_gain]),
        attn_sinks,
        positions[None, :],
        jnp.transpose(router),
        jnp.transpose(expert_ids),
        w_query,
        w_keyvalue.reshape(FULL, 2 * HD),
        jnp.transpose(w_out),
        window_cache.reshape(TOK, LANES, 2 * HD),
        jnp.transpose(gate_up[0], (1, 2, 0)),
        jnp.transpose(w_down[0]),
    )


def solution(mesh):
    in_specs = (
        P("dp", "tp"),
        P(),
        P(None, "tp"),
        P(None, "tp", None),
        P("tp"),
        P("tp", None),
        P("dp", "tp", None, None),
        P("dp"),
        P(),
        P("tp", None),
        P("dp", None, None, "tp"),
        P("dp", None, "tp"),
        P("dp", None),
    )
    out_specs = P("dp", "tp")
    return jax.shard_map(
        on_device, mesh=mesh, in_specs=in_specs, out_specs=out_specs, check_vma=False
    )
```

```python
import math

import jax
import jax.numpy as jnp
from jax import lax
from jax.experimental import pallas as pl
from jax.experimental.pallas import tpu as pltpu
from jax.sharding import PartitionSpec as P

norm_eps = 1e-05
rope_base = 150000.0
glu_alpha = 1.702

COL = 360
PAD = 384
FULL = 2880
NZ = 8
NY = 4
NX = 4
NTP = 2 * NX
SLOTS = 32
GROUP = NY * SLOTS
PAIR = 4
CHUNK = PAIR * SLOTS
PARTS = NY // PAIR
NC = NZ * PARTS
WIDE = NTP * PAD
TOK = 96
HEADS = 4
HD = 64
LANES = 128
SPAN = 8 * TOK
MESH = pl.DeviceIdType.MESH
NT = (((1,), (1,)), ((), ()))
F32 = jnp.float32
BF = jnp.bfloat16


ORDER = (0, 1, 2, 4, 5, 3, 6, 7)
OWN = ORDER.index(0)
SETTLE = 1
AHEAD = 3
STRAIGHT_ROWS = 1
STRAIGHT_ACTS = 0
ON, FAR, GATE, ACT_ON, ACT_FAR, DOWN = 1, 2, 3, 4, 5, 6
STRAIGHT_TOKENS = True


def z_offset(j):
    offset = 0
    for n, value in enumerate(ORDER):
        offset = jnp.where(j == n, value, offset)
    return offset


def dot_nt(a, b):
    return lax.dot_general(a, b, NT, preferred_element_type=F32)


def split3(v):
    hi = v.astype(BF)
    rest = v - hi.astype(F32)
    mid = rest.astype(BF)
    low = (rest - mid.astype(F32)).astype(BF)
    return hi, mid, low


def spread_blocks(src, dst, rows, row_step):
    def part(n, c):
        at = pl.ds(pl.multiple_of(n * row_step, row_step), row_step)
        for b in range(NTP):
            low = b * COL // LANES * LANES
            off = b * COL - low
            high = min(low + 4 * LANES, FULL)
            piece = src[at, low:high]
            dst[at, b * PAD + 2 * LANES : (b + 1) * PAD] = jnp.zeros((row_step, LANES), dst.dtype)
            dst[at, b * PAD : b * PAD + COL] = piece[:, off : off + COL]
        return c

    lax.fori_loop(0, rows // row_step, part, 0)


def layer_body(
    tokens_hbm, again_hbm, mgain_hbm, sinks_hbm, pos_hbm, router_hbm, ids_hbm,
    wq_hbm, wkv_hbm, wo_hbm, cache_hbm, gu_hbm, dn_hbm,
    out,
    rows, acts, wgu, wdn, placed, made, back,
    toks, wq, wkv, wo, cache, raw_gu, raw_dn,
    tokens, again, mgain, sinks, pos, router_t, ids_t, gain_pad, own_gain, tok_pad, qbuf, kvb, scb, resid, hid, placer, comb_hi, comb_lo,
    mine_f, mine_b, sib_b, chip_b, recv_b, table, small, small_t, posb, router_pad, scale_out, scale_in,
    wsem, lsem, d_send, d_recv, r_send, r_recv, x_send, x_recv,
    o_send, o_recv, a_send, a_recv, s_send, s_recv,
):
    dp = lax.axis_index("dp")
    tp = lax.axis_index("tp")
    z, y = lax.div(dp, NY), lax.rem(dp, NY)
    xx, core = lax.div(tp, 2), lax.rem(tp, 2)
    right = lax.rem(xx + 1, NX) * 2 + core
    left = lax.rem(xx + NX - 1, NX) * 2 + core
    across = lax.rem(xx + 2, NX) * 2 + core
    sib = xx * 2 + (1 - core)

    def flip(t):
        return t + 1 - 2 * core

    def cols(t):
        return pl.ds(pl.multiple_of(t * PAD, PAD), PAD)

    barrier = pltpu.get_barrier_semaphore()

    def greet(i, c):
        pl.semaphore_signal(
            barrier, inc=1, device_id=(lax.rem(dp + i, NZ * NY), tp), device_id_type=MESH
        )
        return c

    def greet_tp(i, c):
        pl.semaphore_signal(
            barrier, inc=1, device_id=(dp, lax.rem(tp + i, NTP)), device_id_type=MESH
        )
        return c

    get_small = [
        pltpu.make_async_copy(source, target, wsem.at[28 + n])
        for n, (source, target) in enumerate(
            (
                (tokens_hbm, tokens),
                (pos_hbm, pos),
                (ids_hbm, ids_t),
                (again_hbm, again),
                (mgain_hbm, mgain),
                (router_hbm, router_t),
                (sinks_hbm, sinks),
            )
        )
    ]
    for get in get_small:
        get.start()
    lax.fori_loop(1, NTP, greet_tp, 0)
    lax.fori_loop(1, NZ * NY, greet, 0)

    get_q = [
        pltpu.make_async_copy(
            wq_hbm.at[pl.ds(b * COL, COL), :], wq.at[pl.ds(b * PAD, COL), :], wsem.at[b]
        )
        for b in range(NTP)
    ]
    get_kv = [
        pltpu.make_async_copy(
            wkv_hbm.at[pl.ds(b * COL, COL), :], wkv.at[pl.ds(b * PAD, COL), :], wsem.at[8 + b]
        )
        for b in range(NTP)
    ]
    get_o = [
        pltpu.make_async_copy(
            wo_hbm.at[pl.ds(b * COL, COL), :], wo.at[pl.ds(b * PAD, COL), :], wsem.at[16 + b]
        )
        for b in range(NTP)
    ]
    get_cache = pltpu.make_async_copy(cache_hbm, cache, wsem.at[24])
    get_gu = [
        pltpu.make_async_copy(gu_hbm.at[u], raw_gu.at[pl.ds(u * PAD, COL), :], wsem.at[25 + u])
        for u in range(2)
    ]
    get_dn = pltpu.make_async_copy(dn_hbm, raw_dn.at[pl.ds(0, COL), :], wsem.at[27])
    for group in (get_q, get_kv, [get_cache], get_o, get_gu, [get_dn]):
        for get in group:
            get.start()

    tok_pad[...] = jnp.zeros((TOK, PAD), F32)
    get_small[0].wait()
    tok_pad[:, :COL] = tokens[...].astype(F32)
    toks[0, :, cols(tp)] = tok_pad[...].astype(BF)

    def xcopy(buf, ph, kind, j, part, col, dest):
        ref = buf.at[j, part, cols(col)]
        return pltpu.make_async_remote_copy(
            src_ref=ref,
            dst_ref=ref,
            send_sem=x_send.at[ph, kind, j],
            recv_sem=x_recv.at[ph, kind, j],
            device_id=(dp, dest),
            device_id_type=MESH,
        )

    def parts_of(buf):
        n = buf.shape[1]
        return pl.ds(0, n), pl.ds(0, n // 2), pl.ds(n // 2, n // 2)

    def straight(ph, j):
        if ph == 2:
            return STRAIGHT_TOKENS
        return j < STRAIGHT_ROWS if ph == 0 else j >= NC - STRAIGHT_ACTS

    def send_own(buf, ph, j):
        allr, top, bot = parts_of(buf)

        @pl.when(straight(ph, j))
        def _():
            xcopy(buf, ph, 3, j, allr, tp, across).start()

        xcopy(buf, ph, 0, j, allr, tp, right).start()
        xcopy(buf, ph, 1, j, allr, tp, left).start()
        xcopy(buf, ph, 2, j, allr, tp, sib).start()

    def send_on(buf, ph, j):
        allr, top, bot = parts_of(buf)
        relayed = jnp.logical_not(straight(ph, j))
        xcopy(buf, ph, 0, j, allr, left, right).wait_recv()

        @pl.when(relayed)
        def _():
            xcopy(buf, ph, 3, j, top, left, right).start()

        xcopy(buf, ph, 4, j, allr, left, sib).start()
        xcopy(buf, ph, 1, j, allr, right, left).wait_recv()

        @pl.when(relayed)
        def _():
            xcopy(buf, ph, 5, j, bot, right, left).start()

        xcopy(buf, ph, 6, j, allr, right, sib).start()

    def send_far(buf, ph, j):
        allr, top, bot = parts_of(buf)

        @pl.when(straight(ph, j))
        def _():
            xcopy(buf, ph, 3, j, allr, across, across).wait_recv()

        @pl.when(jnp.logical_not(straight(ph, j)))
        def _():
            xcopy(buf, ph, 3, j, top, across, right).wait_recv()
            xcopy(buf, ph, 5, j, bot, across, left).wait_recv()

        xcopy(buf, ph, 7, j, allr, across, sib).start()

    def all_in(buf, ph, j):
        allr, top, bot = parts_of(buf)
        xcopy(buf, ph, 2, j, allr, sib, sib).wait_recv()
        xcopy(buf, ph, 4, j, allr, flip(left), sib).wait_recv()
        xcopy(buf, ph, 6, j, allr, flip(right), sib).wait_recv()
        xcopy(buf, ph, 7, j, allr, flip(across), sib).wait_recv()

    def all_sent(buf, ph, j):
        allr, top, bot = parts_of(buf)
        for kind in (0, 1, 2, 4, 6, 7):
            xcopy(buf, ph, kind, j, allr, tp, right).wait_send()

        @pl.when(straight(ph, j))
        def _():
            xcopy(buf, ph, 3, j, allr, tp, across).wait_send()

        @pl.when(jnp.logical_not(straight(ph, j)))
        def _():
            xcopy(buf, ph, 3, j, top, left, right).wait_send()
            xcopy(buf, ph, 5, j, bot, right, left).wait_send()

    pl.semaphore_wait(barrier, NZ * NY - 1 + NTP - 1)
    send_own(toks, 2, 0)

    for get in get_small[1:]:
        get.wait()

    for b in range(NTP):
        gain_pad[:, b * PAD + 2 * LANES : (b + 1) * PAD] = jnp.zeros((1, LANES), F32)
        gain_pad[:, b * PAD : b * PAD + COL] = again[b * COL : (b + 1) * COL][None, :]
        own = mgain[b * COL : (b + 1) * COL][None, :]

        @pl.when(tp == b)
        def _():
            own_gain[...] = jnp.zeros((1, PAD), F32)
            own_gain[:, :COL] = own

    small[...] = jnp.zeros((8, LANES), F32)
    small[0:1, :TOK] = pos[...].astype(F32)
    pos_col = jnp.transpose(jnp.broadcast_to(small[0:1, :], (LANES, LANES)))[:TOK]
    lane = lax.broadcasted_iota(jnp.int32, (TOK, LANES), 1)
    inverse = jnp.exp(
        lax.rem(lane, HD // 2).astype(F32) * (-2.0 / HD * math.log(rope_base))
    )
    angles = pos_col * inverse
    first = lax.rem(lane, HD) < HD // 2
    table[0] = jnp.cos(angles)
    sine = jnp.sin(angles)
    table[1] = jnp.where(first, -sine, sine)
    for g in range(8):
        posb[pl.ds(g, TOK, stride=8), :] = pos_col

    experts = NZ * NY
    e_iota = lax.broadcasted_iota(jnp.int32, (experts, TOK), 0)
    named = e_iota == ids_t[0:1, :]
    for k in range(1, ids_t.shape[0]):
        named = named | (e_iota == ids_t[k : k + 1, :])
    before = (
        lax.broadcasted_iota(jnp.int32, (TOK, TOK), 0)
        < lax.broadcasted_iota(jnp.int32, (TOK, TOK), 1)
    ).astype(F32)
    named_f = named.astype(F32)
    router_pad[...] = jnp.zeros((experts, PAD), BF)
    router_pad[:, :COL] = router_t[...]
    slot = jnp.dot(named_f, before, preferred_element_type=F32)
    slot = jnp.where(named, slot, -1.0)
    s_iota = lax.broadcasted_iota(jnp.int32, (SLOTS, TOK), 0).astype(F32)
    for e in range(experts):
        placer[e * SLOTS : (e + 1) * SLOTS, :] = (
            s_iota == slot[e : e + 1, :]
        ).astype(F32)

    send_on(toks, 2, 0)
    send_far(toks, 2, 0)
    for group, ref in ((get_q, wq), (get_kv, wkv), (get_o, wo)):
        for b, get in enumerate(group):
            get.wait()
            ref[b * PAD + COL : (b + 1) * PAD, :] = jnp.zeros((PAD - COL, ref.shape[1]), BF)
    all_in(toks, 2, 0)

    wide = toks[0].astype(F32)
    mean = jnp.sum(wide * wide, axis=1, keepdims=True) * (1.0 / FULL)
    normed = (wide * lax.rsqrt(mean + norm_eps) * gain_pad[...]).astype(BF)
    queries = jnp.dot(normed, wq[...], preferred_element_type=F32)
    fresh = jnp.dot(normed, wkv[...], preferred_element_type=F32)

    def turned(v):
        swapped = jnp.where(
            first, pltpu.roll(v, LANES - HD // 2, axis=1), pltpu.roll(v, HD // 2, axis=1)
        )
        return v * table[0] + swapped * table[1]

    entry = jnp.where(lane < HD, turned(fresh), fresh).astype(BF).astype(F32)
    qbuf[...] = jnp.zeros((SPAN, LANES), F32)
    kvb[...] = jnp.zeros((SPAN, LANES), F32)
    for g in range(HEADS):
        tile = g // 2
        if g % 2 == 0:
            rotated = turned(queries[:, tile * LANES : (tile + 1) * LANES]).astype(BF).astype(F32)
        head = rotated if g % 2 == 0 else pltpu.roll(rotated, HD, axis=1)
        qbuf[pl.ds(g, TOK, stride=8), :] = jnp.where(lane < HD, head * HD**-0.5, 0.0)
        kvb[pl.ds(g, TOK, stride=8), :] = entry
    get_cache.wait()

    sub = lax.broadcasted_iota(jnp.int32, (8, LANES), 0)
    sink = jnp.where(
        sub == 0,
        sinks[0],
        jnp.where(sub == 1, sinks[1], jnp.where(sub == 2, sinks[2], sinks[3])),
    )[:, :1]
    group = 48
    sink = jnp.concatenate([sink] * group, axis=0)
    slots = lax.broadcasted_iota(jnp.int32, (8 * group, LANES), 1)

    empty = jnp.zeros((8, LANES), F32)

    def apart(two):
        upper = jnp.concatenate([two[:8], empty], axis=1)
        lower = jnp.concatenate([empty, two[8:]], axis=1)
        return jnp.concatenate([upper, lower], axis=0).astype(BF)

    def both(s):
        return jnp.concatenate([cache[s], cache[s + 1]], axis=1)

    def attend(n, c):
        at = pl.ds(pl.multiple_of(n * 8 * group, 8 * group), 8 * group)
        asked = qbuf[at, :]
        entries = kvb[at, :]
        where_now = posb[at, :].astype(jnp.int32)
        newest = jnp.sum(asked * entries, axis=1, keepdims=True)
        raw = jnp.concatenate(
            [
                dot_nt(apart(asked[8 * u : 8 * u + 16]), both(n * group + u))
                for u in range(0, group, 2)
            ],
            axis=0,
        )
        current = slots == lax.rem(where_now, LANES)
        raw = jnp.where(current, newest, raw)
        raw = jnp.where(slots <= where_now, raw, -jnp.inf)
        peak = jnp.maximum(jnp.max(raw, axis=1, keepdims=True), sink)
        raised = jnp.exp(raw - peak)
        total = jnp.sum(raised, axis=1, keepdims=True) + jnp.exp(sink - peak)
        probs = (raised / total).astype(BF).astype(F32)
        newest_prob = (jnp.exp(newest - peak) / total).astype(BF).astype(F32)
        kept = jnp.where(current, 0.0, probs)
        mixed = []
        for u in range(0, group, 2):
            pair = jnp.dot(
                kept[8 * u : 8 * u + 16].astype(BF),
                both(n * group + u),
                preferred_element_type=F32,
            )
            mixed += [pair[:8, :LANES], pair[8:, LANES:]]
        mixed = jnp.concatenate(mixed, axis=0)
        scb[at, :] = mixed + newest_prob * entries
        return c

    lax.fori_loop(0, TOK // group, attend, 0)
    tiles = []
    for tile in range(2):
        even = scb[pl.ds(2 * tile, TOK, stride=8), :]
        odd = scb[pl.ds(2 * tile + 1, TOK, stride=8), :]
        tiles.append(jnp.where(lane < HD, pltpu.roll(even, HD, axis=1), odd).astype(BF))
    attended = jnp.concatenate(tiles, axis=1)

    def out_block(owner):
        return dot_nt(attended, wo[cols(owner), :])

    for n in range(NX):
        mine_b[n] = out_block(2 * n + 1 - core).astype(BF)
    to_sib = pltpu.make_async_remote_copy(
        src_ref=mine_b,
        dst_ref=sib_b,
        send_sem=o_send.at[0],
        recv_sem=o_recv.at[0],
        device_id=(dp, sib),
        device_id_type=MESH,
    )
    to_sib.start()
    for n in range(NX):
        mine_f[n] = out_block(2 * n + core)
    to_sib.wait_recv()

    def to_chip(i):
        owner = lax.rem(xx + i, NX)
        return pltpu.make_async_remote_copy(
            src_ref=chip_b.at[owner],
            dst_ref=recv_b.at[i],
            send_sem=o_send.at[i],
            recv_sem=o_recv.at[i],
            device_id=(dp, owner * 2 + core),
            device_id_type=MESH,
        )

    for i in (2, 1, 3):
        owner = lax.rem(xx + i, NX)
        chip_b[owner] = (mine_f[owner] + sib_b[owner].astype(F32)).astype(BF)
        to_chip(i).start()
    total = tok_pad[...] + (mine_f[xx] + sib_b[xx].astype(F32))
    for get in get_gu:
        get.wait()
    raw_gu[COL:PAD, :] = jnp.zeros((PAD - COL, FULL), BF)
    raw_gu[PAD + COL : 2 * PAD, :] = jnp.zeros((PAD - COL, FULL), BF)
    spread_blocks(raw_gu, wgu, 2 * PAD, 48)
    get_dn.wait()
    raw_dn[COL:PAD, :] = jnp.zeros((PAD - COL, FULL), BF)
    spread_blocks(raw_dn, wdn, PAD, 48)
    for i in (1, 3, 2):
        to_chip(i).wait_recv()
    for i in (1, 2, 3):
        total = total + recv_b[i].astype(F32)
    resid[...] = total

    hid[...] = (total * own_gain[...]).astype(BF)

    def within(i):
        return pl.ds(pl.multiple_of(lax.rem(i, PAIR) * SLOTS, SLOTS), SLOTS)

    def dispatch_copy(j, i):
        dest = lax.rem(z + NZ + NZ - z_offset(j), NZ) * NY + lax.rem(y + NY - i, NY)
        return pltpu.make_async_remote_copy(
            src_ref=placed.at[pl.ds(pl.multiple_of(dest * SLOTS, SLOTS), SLOTS), :],
            dst_ref=rows.at[j * PARTS + lax.div(i, PAIR), within(i), cols(tp)],
            send_sem=d_send.at[j * NY + i],
            recv_sem=d_recv.at[j * NY + i],
            device_id=(dest, tp),
            device_id_type=MESH,
        )

    own_in = pltpu.make_async_copy(
        placed.at[pl.ds(pl.multiple_of(dp * SLOTS, SLOTS), SLOTS), :],
        rows.at[OWN * PARTS, pl.ds(0, SLOTS), cols(tp)],
        lsem.at[0],
    )

    def dispatch(j, c):
        zd = lax.rem(z + NZ + NZ - z_offset(j), NZ)
        part = pl.ds(pl.multiple_of(zd * GROUP, GROUP), GROUP)
        placed[part, :] = jnp.dot(
            placer[part, :].astype(BF), hid[...], preferred_element_type=F32
        ).astype(BF)

        @pl.when(j == OWN)
        def _():
            own_in.start()

        @pl.when(j != OWN)
        def _():
            dispatch_copy(j, 0).start()

        for i in range(1, NY):
            dispatch_copy(j, i).start()
        return c

    lax.fori_loop(0, AHEAD, dispatch, 0)

    lifted = total * own_gain[...]
    wide_rows = jnp.zeros((LANES - TOK, PAD), BF)
    logit_part = jnp.zeros((experts, LANES), F32)
    for piece in split3(lifted):
        logit_part = logit_part + dot_nt(router_pad[...], jnp.concatenate([piece, wide_rows], axis=0))
    square_part = jnp.zeros((8, LANES), F32)
    ones = jnp.ones((8, PAD), BF)
    for piece in split3(total * total):
        square_part = square_part + dot_nt(ones, jnp.concatenate([piece, wide_rows], axis=0))
    small_t[tp, 0:experts, :] = logit_part
    small_t[tp, experts : experts + 8, :] = square_part

    def share(i):
        return pltpu.make_async_remote_copy(
            src_ref=small_t.at[tp],
            dst_ref=small_t.at[tp],
            send_sem=a_send.at[i],
            recv_sem=a_recv.at[i],
            device_id=(dp, lax.rem(tp + i, NTP)),
            device_id_type=MESH,
        )

    for i in range(1, NTP):
        share(i).start()

    def scale_copy(j, i):
        zd = lax.rem(z + NZ - z_offset(j), NZ)
        dest = zd * NY + lax.rem(y + NY - i, NY)
        return pltpu.make_async_remote_copy(
            src_ref=scale_out.at[zd],
            dst_ref=scale_in.at[j * NY + i],
            send_sem=s_send.at[j * NY + i],
            recv_sem=s_recv.at[j * NY + i],
            device_id=(dest, tp),
            device_id_type=MESH,
        )

    def scales_of(c):
        spot = lax.broadcasted_iota(jnp.int32, (1, LANES), 1)
        line = jnp.zeros((1, LANES), F32)
        for k in range(PAIR):
            n = c * PAIR + k

            @pl.when(n != OWN * NY)
            def _():
                scale_copy(lax.div(n, NY), lax.rem(n, NY)).wait_recv()

            there = pltpu.roll(
                jnp.broadcast_to(scale_in[n], (8, LANES)),
                lax.rem(k + NY - y, NY) * SLOTS,
                axis=1,
            )[0:1]
            line = jnp.where(lax.div(spot, SLOTS) == k, there, line)
        return jnp.transpose(jnp.broadcast_to(line, (LANES, LANES)))[:CHUNK, :1]

    def sums():
        summed = small_t[0]
        for n in range(1, NTP):
            summed = summed + small_t[n]
        scale_row = lax.rsqrt(summed[experts : experts + 1, :] * (1.0 / FULL) + norm_eps)
        return summed, scale_row

    def settle():
        for i in range(1, NTP):
            share(i).wait_recv()
        scale_row = sums()[1]
        hi, mid, low = split3(jnp.broadcast_to(scale_row[:, :TOK], (8, TOK)))
        which = lax.broadcasted_iota(jnp.int32, (8, TOK), 0)
        stacked = jnp.where(
            which == 0,
            hi.astype(F32),
            jnp.where(which == 1, mid.astype(F32), jnp.where(which == 2, low.astype(F32), 0.0)),
        ).astype(BF)
        for n in range(NZ):
            at = slice(n * GROUP, (n + 1) * GROUP)
            spots = placer[at, :].astype(BF)
            scale_out[n] = jnp.sum(dot_nt(stacked, spots), axis=0, keepdims=True)
        scale_in[OWN * NY] = scale_out[z]

        def send_scale(n, c):
            j, i = lax.div(n, NY), lax.rem(n, NY)

            @pl.when(n != OWN * NY)
            def _():
                scale_copy(j, i).start()

            return c

        lax.fori_loop(0, NZ * NY, send_scale, 0)

    def combine_weights():
        summed, scale_row = sums()
        logits = summed[0:experts, :TOK] * scale_row[:, :TOK]
        lifted_logits = jnp.where(named, jnp.exp(logits), 0.0)
        weights = lifted_logits / jnp.sum(lifted_logits, axis=0, keepdims=True)
        for e in range(experts):
            at = slice(e * SLOTS, (e + 1) * SLOTS)
            placer[at, :] = placer[at, :] * weights[e : e + 1, :]
        for n in range(NZ):
            at = slice(n * GROUP, (n + 1) * GROUP)
            piece = jnp.transpose(placer[at, :])
            hi = piece.astype(BF)
            comb_hi[:, at] = hi
            comb_lo[:, at] = (piece - hi.astype(F32)).astype(BF)

    def back_copy(j, i):
        home = lax.rem(z + z_offset(j), NZ) * NY + lax.rem(y + i, NY)
        return pltpu.make_async_remote_copy(
            src_ref=made.at[j * PARTS + lax.div(i, PAIR), within(i), :],
            dst_ref=back.at[pl.ds(pl.multiple_of(dp * SLOTS, SLOTS), SLOTS), :],
            send_sem=r_send.at[j * NY + i],
            recv_sem=r_recv.at[dp],
            device_id=(home, tp),
            device_id_type=MESH,
        )

    own_back = pltpu.make_async_copy(
        made.at[OWN * PARTS, pl.ds(0, SLOTS), :],
        back.at[pl.ds(pl.multiple_of(dp * SLOTS, SLOTS), SLOTS), :],
        lsem.at[1],
    )

    def step(t, c):
        @pl.when(t < NC)
        def _():
            for k in range(PAIR):
                n = t * PAIR + k

                @pl.when(n == OWN * NY)
                def _():
                    own_in.wait()

                @pl.when(n != OWN * NY)
                def _():
                    dispatch_copy(lax.div(n, NY), lax.rem(n, NY)).wait_recv()

            send_own(rows, 0, t)

        @pl.when(t == SETTLE)
        def _():
            settle()

        @pl.when((t >= ON) & (t < NC + ON))
        def _():
            send_on(rows, 0, t - ON)

        @pl.when((lax.rem(t, PARTS) == 0) & (t < (NZ - AHEAD) * PARTS))
        def _():
            dispatch(lax.div(t, PARTS) + AHEAD, 0)

        @pl.when((t >= GATE) & (t < NC + GATE))
        def _():
            j = t - GATE
            scales = scales_of(j)
            all_in(rows, 0, j)
            mixed = dot_nt(rows[j], wgu[...]) * scales
            gate = mixed[:, :PAD]
            up = mixed[:, PAD:]
            act = gate * jax.nn.sigmoid(glu_alpha * gate) * (up + 1.0)
            acts[j, :, cols(tp)] = act.astype(BF)
            send_own(acts, 1, j)

        @pl.when((t >= FAR) & (t < NC + FAR))
        def _():
            send_far(rows, 0, t - FAR)

        @pl.when((t >= ACT_ON) & (t < NC + ACT_ON))
        def _():
            send_on(acts, 1, t - ACT_ON)

        @pl.when(t == (NZ - AHEAD) * PARTS + 1)
        def _():
            combine_weights()

        @pl.when((t >= DOWN) & (t < NC + DOWN))
        def _():
            j = t - DOWN
            all_in(acts, 1, j)
            made[j] = dot_nt(acts[j], wdn[...]).astype(BF)
            for k in range(PAIR):
                n = j * PAIR + k

                @pl.when(n == OWN * NY)
                def _():
                    own_back.start()

                @pl.when(n != OWN * NY)
                def _():
                    back_copy(lax.div(n, NY), lax.rem(n, NY)).start()

        @pl.when((t >= ACT_FAR) & (t < NC + ACT_FAR))
        def _():
            send_far(acts, 1, t - ACT_FAR)

        return c

    lax.fori_loop(0, NC + DOWN, step, 0)

    to_sib.wait_send()
    for i in range(1, NX):
        to_chip(i).wait_send()
    for i in range(1, NTP):
        share(i).wait_send()
    all_sent(toks, 2, 0)

    def sent(n, c):
        @pl.when(n != OWN * NY)
        def _():
            j, i = lax.div(n, NY), lax.rem(n, NY)
            dispatch_copy(j, i).wait_send()
            back_copy(j, i).wait_send()
            scale_copy(j, i).wait_send()

        return c

    lax.fori_loop(0, NZ * NY, sent, 0)

    def sent_x(j, c):
        all_sent(rows, 0, j)
        all_sent(acts, 1, j)
        return c

    lax.fori_loop(0, NC, sent_x, 0)

    def await_back(i, c):
        peer = lax.rem(dp + i, NZ * NY)
        pltpu.make_async_remote_copy(
            src_ref=made.at[0, pl.ds(0, SLOTS), :],
            dst_ref=back.at[pl.ds(pl.multiple_of(peer * SLOTS, SLOTS), SLOTS), :],
            send_sem=r_send.at[1],
            recv_sem=r_recv.at[peer],
            device_id=(peer, tp),
            device_id_type=MESH,
        ).wait_recv()
        return c

    own_back.wait()
    lax.fori_loop(1, NZ * NY, await_back, 0)
    got = back[...]
    answer = (
        resid[...]
        + jnp.dot(comb_hi[...], got, preferred_element_type=F32)
        + jnp.dot(comb_lo[...], got, preferred_element_type=F32)
    )
    out[...] = answer[:, :COL]


def on_device(
    tokens,
    attn_gain,
    w_query,
    w_keyvalue,
    attn_sinks,
    w_out,
    window_cache,
    positions,
    moe_gain,
    router,
    gate_up,
    w_down,
    expert_ids,
):
    vmem = pl.BlockSpec(memory_space=pltpu.VMEM)
    hbm = pl.BlockSpec(memory_space=pl.ANY)
    dma = pltpu.SemaphoreType.DMA
    vm = pltpu.VMEM
    return pl.pallas_call(
        layer_body,
        out_shape=jax.ShapeDtypeStruct(tokens.shape, F32),
        in_specs=[hbm] * 13,
        out_specs=vmem,
        scratch_shapes=[
            vm((NC, CHUNK, WIDE), BF),
            vm((NC, CHUNK, WIDE), BF),
            vm((2 * PAD, WIDE), BF),
            vm((PAD, WIDE), BF),
            vm((NZ * GROUP, PAD), BF),
            vm((NC, CHUNK, PAD), BF),
            vm((NZ * GROUP, PAD), BF),
            vm((1, TOK, WIDE), BF),
            vm((WIDE, HEADS * HD), BF),
            vm((WIDE, 2 * HD), BF),
            vm((WIDE, HEADS * HD), BF),
            vm((TOK, LANES, 2 * HD), BF),
            vm((2 * PAD, FULL), BF),
            vm((PAD, FULL), BF),
            vm((TOK, COL), BF),
            vm((FULL,), F32),
            vm((FULL,), F32),
            pltpu.SMEM((HEADS,), F32),
            vm((1, TOK), jnp.int32),
            vm((NZ * NY, COL), BF),
            vm((expert_ids.shape[1], TOK), jnp.int32),
            vm((1, WIDE), F32),
            vm((1, PAD), F32),
            vm((TOK, PAD), F32),
            vm((SPAN, LANES), F32),
            vm((SPAN, LANES), F32),
            vm((SPAN, LANES), F32),
            vm((TOK, PAD), F32),
            vm((TOK, PAD), BF),
            vm((NZ * GROUP, TOK), F32),
            vm((TOK, NZ * GROUP), BF),
            vm((TOK, NZ * GROUP), BF),
            vm((NX, TOK, PAD), F32),
            vm((NX, TOK, PAD), BF),
            vm((NX, TOK, PAD), BF),
            vm((NX, TOK, PAD), BF),
            vm((NX, TOK, PAD), BF),
            vm((2, TOK, LANES), F32),
            vm((8, LANES), F32),
            vm((NTP, 40, LANES), F32),
            vm((SPAN, LANES), F32),
            vm((NZ * NY, PAD), BF),
            vm((NZ, 1, LANES), F32),
            vm((NZ * NY, 1, LANES), F32),
            dma((35,)),
            dma((2,)),
            dma((NZ * NY,)),
            dma((NZ * NY,)),
            dma((NZ * NY,)),
            dma((NZ * NY,)),
            dma((3, 8, NC)),
            dma((3, 8, NC)),
            dma((NX,)),
            dma((NX,)),
            dma((NTP,)),
            dma((NTP,)),
            dma((NZ * NY,)),
            dma((NZ * NY,)),
        ],
        compiler_params=pltpu.CompilerParams(
            collective_id=0, has_side_effects=True, vmem_limit_bytes=60 * 1024 * 1024
        ),
        name="layer",
    )(
        tokens,
        attn_gain,
        moe_gain,
        attn_sinks,
        positions[None, :],
        jnp.transpose(router),
        jnp.transpose(expert_ids),
        w_query,
        w_keyvalue.reshape(FULL, 2 * HD),
        jnp.transpose(w_out),
        window_cache.reshape(TOK, LANES, 2 * HD),
        jnp.transpose(gate_up[0], (1, 2, 0)),
        jnp.transpose(w_down[0]),
    )


def solution(mesh):
    in_specs = (
        P("dp", "tp"),
        P(),
        P(None, "tp"),
        P(None, "tp", None),
        P("tp"),
        P("tp", None),
        P("dp", "tp", None, None),
        P("dp"),
        P(),
        P("tp", None),
        P("dp", None, None, "tp"),
        P("dp", None, "tp"),
        P("dp", None),
    )
    out_specs = P("dp", "tp")
    return jax.shard_map(
        on_device, mesh=mesh, in_specs=in_specs, out_specs=out_specs, check_vma=False
    )
```

```python
import math

import jax
import jax.numpy as jnp
from jax import lax
from jax.experimental import pallas as pl
from jax.experimental.pallas import tpu as pltpu
from jax.sharding import PartitionSpec as P

norm_eps = 1e-05
rope_base = 150000.0
glu_alpha = 1.702

COL = 360
PAD = 384
FULL = 2880
NZ = 8
NY = 4
NX = 4
NTP = 2 * NX
SLOTS = 32
GROUP = NY * SLOTS
PAIR = 4
CHUNK = PAIR * SLOTS
PARTS = NY // PAIR
NC = NZ * PARTS
WIDE = NTP * PAD
TOK = 96
HEADS = 4
HD = 64
LANES = 128
SPAN = 8 * TOK
MESH = pl.DeviceIdType.MESH
NT = (((1,), (1,)), ((), ()))
F32 = jnp.float32
BF = jnp.bfloat16


ORDER = (0, 7, 2, 4, 3, 5, 6, 1)
OWN = ORDER.index(0)
SETTLE = 1
AHEAD = 3
STRAIGHT_ROWS = 1
STRAIGHT_ACTS = 0
ON, FAR, GATE, ACT_ON, ACT_FAR, DOWN = 1, 2, 3, 4, 5, 6
STRAIGHT_TOKENS = True


def z_offset(j):
    offset = 0
    for n, value in enumerate(ORDER):
        offset = jnp.where(j == n, value, offset)
    return offset


def dot_nt(a, b):
    return lax.dot_general(a, b, NT, preferred_element_type=F32)


def split3(v):
    hi = v.astype(BF)
    rest = v - hi.astype(F32)
    mid = rest.astype(BF)
    low = (rest - mid.astype(F32)).astype(BF)
    return hi, mid, low


def spread_blocks(src, dst, rows, row_step):
    def part(n, c):
        at = pl.ds(pl.multiple_of(n * row_step, row_step), row_step)
        for b in range(NTP):
            low = b * COL // LANES * LANES
            off = b * COL - low
            high = min(low + 4 * LANES, FULL)
            piece = src[at, low:high]
            dst[at, b * PAD + 2 * LANES : (b + 1) * PAD] = jnp.zeros((row_step, LANES), dst.dtype)
            dst[at, b * PAD : b * PAD + COL] = piece[:, off : off + COL]
        return c

    lax.fori_loop(0, rows // row_step, part, 0)


def layer_body(
    tokens_hbm, again_hbm, mgain_hbm, sinks_hbm, pos_hbm, router_hbm, ids_hbm,
    wq_hbm, wkv_hbm, wo_hbm, cache_hbm, gu_hbm, dn_hbm,
    out,
    rows, acts, wgu, wdn, placed, made, back,
    toks, wq, wkv, wo, cache, raw_gu, raw_dn,
    tokens, again, mgain, sinks, pos, router_t, ids_t, gain_pad, own_gain, tok_pad, qbuf, kvb, scb, resid, hid, placer, comb_hi, comb_lo,
    mine_f, mine_b, sib_b, chip_b, recv_b, table, small, small_t, posb, router_pad, scale_out, scale_in,
    wsem, lsem, d_send, d_recv, r_send, r_recv, x_send, x_recv,
    o_send, o_recv, a_send, a_recv, s_send, s_recv,
):
    dp = lax.axis_index("dp")
    tp = lax.axis_index("tp")
    z, y = lax.div(dp, NY), lax.rem(dp, NY)
    xx, core = lax.div(tp, 2), lax.rem(tp, 2)
    right = lax.rem(xx + 1, NX) * 2 + core
    left = lax.rem(xx + NX - 1, NX) * 2 + core
    across = lax.rem(xx + 2, NX) * 2 + core
    sib = xx * 2 + (1 - core)

    def flip(t):
        return t + 1 - 2 * core

    def cols(t):
        return pl.ds(pl.multiple_of(t * PAD, PAD), PAD)

    barrier = pltpu.get_barrier_semaphore()

    def greet(i, c):
        pl.semaphore_signal(
            barrier, inc=1, device_id=(lax.rem(dp + i, NZ * NY), tp), device_id_type=MESH
        )
        return c

    def greet_tp(i, c):
        pl.semaphore_signal(
            barrier, inc=1, device_id=(dp, lax.rem(tp + i, NTP)), device_id_type=MESH
        )
        return c

    get_small = [
        pltpu.make_async_copy(source, target, wsem.at[28 + n])
        for n, (source, target) in enumerate(
            (
                (tokens_hbm, tokens),
                (pos_hbm, pos),
                (ids_hbm, ids_t),
                (again_hbm, again),
                (mgain_hbm, mgain),
                (router_hbm, router_t),
                (sinks_hbm, sinks),
            )
        )
    ]
    for get in get_small:
        get.start()
    lax.fori_loop(1, NTP, greet_tp, 0)
    lax.fori_loop(1, NZ * NY, greet, 0)

    get_q = [
        pltpu.make_async_copy(
            wq_hbm.at[pl.ds(b * COL, COL), :], wq.at[pl.ds(b * PAD, COL), :], wsem.at[b]
        )
        for b in range(NTP)
    ]
    get_kv = [
        pltpu.make_async_copy(
            wkv_hbm.at[pl.ds(b * COL, COL), :], wkv.at[pl.ds(b * PAD, COL), :], wsem.at[8 + b]
        )
        for b in range(NTP)
    ]
    get_o = [
        pltpu.make_async_copy(
            wo_hbm.at[pl.ds(b * COL, COL), :], wo.at[pl.ds(b * PAD, COL), :], wsem.at[16 + b]
        )
        for b in range(NTP)
    ]
    get_cache = pltpu.make_async_copy(cache_hbm, cache, wsem.at[24])
    get_gu = [
        pltpu.make_async_copy(gu_hbm.at[u], raw_gu.at[pl.ds(u * PAD, COL), :], wsem.at[25 + u])
        for u in range(2)
    ]
    get_dn = pltpu.make_async_copy(dn_hbm, raw_dn.at[pl.ds(0, COL), :], wsem.at[27])
    for group in (get_q, get_kv, [get_cache], get_o, get_gu, [get_dn]):
        for get in group:
            get.start()

    tok_pad[...] = jnp.zeros((TOK, PAD), F32)
    get_small[0].wait()
    tok_pad[:, :COL] = tokens[...].astype(F32)
    toks[0, :, cols(tp)] = tok_pad[...].astype(BF)

    def xcopy(buf, ph, kind, j, part, col, dest):
        ref = buf.at[j, part, cols(col)]
        return pltpu.make_async_remote_copy(
            src_ref=ref,
            dst_ref=ref,
            send_sem=x_send.at[ph, kind, j],
            recv_sem=x_recv.at[ph, kind, j],
            device_id=(dp, dest),
            device_id_type=MESH,
        )

    def parts_of(buf):
        n = buf.shape[1]
        return pl.ds(0, n), pl.ds(0, n // 2), pl.ds(n // 2, n // 2)

    def straight(ph, j):
        if ph == 2:
            return STRAIGHT_TOKENS
        return j < STRAIGHT_ROWS if ph == 0 else j >= NC - STRAIGHT_ACTS

    def send_own(buf, ph, j):
        allr, top, bot = parts_of(buf)

        @pl.when(straight(ph, j))
        def _():
            xcopy(buf, ph, 3, j, allr, tp, across).start()

        xcopy(buf, ph, 0, j, allr, tp, right).start()
        xcopy(buf, ph, 1, j, allr, tp, left).start()
        xcopy(buf, ph, 2, j, allr, tp, sib).start()

    def send_on(buf, ph, j):
        allr, top, bot = parts_of(buf)
        relayed = jnp.logical_not(straight(ph, j))
        xcopy(buf, ph, 0, j, allr, left, right).wait_recv()

        @pl.when(relayed)
        def _():
            xcopy(buf, ph, 3, j, top, left, right).start()

        xcopy(buf, ph, 4, j, allr, left, sib).start()
        xcopy(buf, ph, 1, j, allr, right, left).wait_recv()

        @pl.when(relayed)
        def _():
            xcopy(buf, ph, 5, j, bot, right, left).start()

        xcopy(buf, ph, 6, j, allr, right, sib).start()

    def send_far(buf, ph, j):
        allr, top, bot = parts_of(buf)

        @pl.when(straight(ph, j))
        def _():
            xcopy(buf, ph, 3, j, allr, across, across).wait_recv()

        @pl.when(jnp.logical_not(straight(ph, j)))
        def _():
            xcopy(buf, ph, 3, j, top, across, right).wait_recv()
            xcopy(buf, ph, 5, j, bot, across, left).wait_recv()

        xcopy(buf, ph, 7, j, allr, across, sib).start()

    def all_in(buf, ph, j):
        allr, top, bot = parts_of(buf)
        xcopy(buf, ph, 2, j, allr, sib, sib).wait_recv()
        xcopy(buf, ph, 4, j, allr, flip(left), sib).wait_recv()
        xcopy(buf, ph, 6, j, allr, flip(right), sib).wait_recv()
        xcopy(buf, ph, 7, j, allr, flip(across), sib).wait_recv()

    def all_sent(buf, ph, j):
        allr, top, bot = parts_of(buf)
        for kind in (0, 1, 2, 4, 6, 7):
            xcopy(buf, ph, kind, j, allr, tp, right).wait_send()

        @pl.when(straight(ph, j))
        def _():
            xcopy(buf, ph, 3, j, allr, tp, across).wait_send()

        @pl.when(jnp.logical_not(straight(ph, j)))
        def _():
            xcopy(buf, ph, 3, j, top, left, right).wait_send()
            xcopy(buf, ph, 5, j, bot, right, left).wait_send()

    pl.semaphore_wait(barrier, NZ * NY - 1 + NTP - 1)
    send_own(toks, 2, 0)

    for get in get_small[1:]:
        get.wait()

    for b in range(NTP):
        gain_pad[:, b * PAD + 2 * LANES : (b + 1) * PAD] = jnp.zeros((1, LANES), F32)
        gain_pad[:, b * PAD : b * PAD + COL] = again[b * COL : (b + 1) * COL][None, :]
        own = mgain[b * COL : (b + 1) * COL][None, :]

        @pl.when(tp == b)
        def _():
            own_gain[...] = jnp.zeros((1, PAD), F32)
            own_gain[:, :COL] = own

    small[...] = jnp.zeros((8, LANES), F32)
    small[0:1, :TOK] = pos[...].astype(F32)
    pos_col = jnp.transpose(jnp.broadcast_to(small[0:1, :], (LANES, LANES)))[:TOK]
    lane = lax.broadcasted_iota(jnp.int32, (TOK, LANES), 1)
    inverse = jnp.exp(
        lax.rem(lane, HD // 2).astype(F32) * (-2.0 / HD * math.log(rope_base))
    )
    angles = pos_col * inverse
    first = lax.rem(lane, HD) < HD // 2
    table[0] = jnp.cos(angles)
    sine = jnp.sin(angles)
    table[1] = jnp.where(first, -sine, sine)
    for g in range(8):
        posb[pl.ds(g, TOK, stride=8), :] = pos_col

    experts = NZ * NY
    e_iota = lax.broadcasted_iota(jnp.int32, (experts, TOK), 0)
    named = e_iota == ids_t[0:1, :]
    for k in range(1, ids_t.shape[0]):
        named = named | (e_iota == ids_t[k : k + 1, :])
    before = (
        lax.broadcasted_iota(jnp.int32, (TOK, TOK), 0)
        < lax.broadcasted_iota(jnp.int32, (TOK, TOK), 1)
    ).astype(F32)
    named_f = named.astype(F32)
    router_pad[...] = jnp.zeros((experts, PAD), BF)
    router_pad[:, :COL] = router_t[...]
    slot = jnp.dot(named_f, before, preferred_element_type=F32)
    slot = jnp.where(named, slot, -1.0)
    s_iota = lax.broadcasted_iota(jnp.int32, (SLOTS, TOK), 0).astype(F32)
    for e in range(experts):
        placer[e * SLOTS : (e + 1) * SLOTS, :] = (
            s_iota == slot[e : e + 1, :]
        ).astype(F32)

    send_on(toks, 2, 0)
    send_far(toks, 2, 0)
    for group, ref in ((get_q, wq), (get_kv, wkv), (get_o, wo)):
        for b, get in enumerate(group):
            get.wait()
            ref[b * PAD + COL : (b + 1) * PAD, :] = jnp.zeros((PAD - COL, ref.shape[1]), BF)
    all_in(toks, 2, 0)

    wide = toks[0].astype(F32)
    mean = jnp.sum(wide * wide, axis=1, keepdims=True) * (1.0 / FULL)
    normed = (wide * lax.rsqrt(mean + norm_eps) * gain_pad[...]).astype(BF)
    queries = jnp.dot(normed, wq[...], preferred_element_type=F32)
    fresh = jnp.dot(normed, wkv[...], preferred_element_type=F32)

    def turned(v):
        swapped = jnp.where(
            first, pltpu.roll(v, LANES - HD // 2, axis=1), pltpu.roll(v, HD // 2, axis=1)
        )
        return v * table[0] + swapped * table[1]

    entry = jnp.where(lane < HD, turned(fresh), fresh).astype(BF).astype(F32)
    qbuf[...] = jnp.zeros((SPAN, LANES), F32)
    kvb[...] = jnp.zeros((SPAN, LANES), F32)
    for g in range(HEADS):
        tile = g // 2
        if g % 2 == 0:
            rotated = turned(queries[:, tile * LANES : (tile + 1) * LANES]).astype(BF).astype(F32)
        head = rotated if g % 2 == 0 else pltpu.roll(rotated, HD, axis=1)
        qbuf[pl.ds(g, TOK, stride=8), :] = jnp.where(lane < HD, head * HD**-0.5, 0.0)
        kvb[pl.ds(g, TOK, stride=8), :] = entry
    get_cache.wait()

    sub = lax.broadcasted_iota(jnp.int32, (8, LANES), 0)
    sink = jnp.where(
        sub == 0,
        sinks[0],
        jnp.where(sub == 1, sinks[1], jnp.where(sub == 2, sinks[2], sinks[3])),
    )[:, :1]
    group = 96
    sink = jnp.concatenate([sink] * group, axis=0)
    slots = lax.broadcasted_iota(jnp.int32, (8 * group, LANES), 1)

    empty = jnp.zeros((8, LANES), F32)

    def apart(two):
        upper = jnp.concatenate([two[:8], empty], axis=1)
        lower = jnp.concatenate([empty, two[8:]], axis=1)
        return jnp.concatenate([upper, lower], axis=0).astype(BF)

    def both(s):
        return jnp.concatenate([cache[s], cache[s + 1]], axis=1)

    def attend(n, c):
        at = pl.ds(pl.multiple_of(n * 8 * group, 8 * group), 8 * group)
        asked = qbuf[at, :]
        entries = kvb[at, :]
        where_now = posb[at, :].astype(jnp.int32)
        newest = jnp.sum(asked * entries, axis=1, keepdims=True)
        raw = jnp.concatenate(
            [
                dot_nt(apart(asked[8 * u : 8 * u + 16]), both(n * group + u))
                for u in range(0, group, 2)
            ],
            axis=0,
        )
        current = slots == lax.rem(where_now, LANES)
        raw = jnp.where(current, newest, raw)
        raw = jnp.where(slots <= where_now, raw, -jnp.inf)
        peak = jnp.maximum(jnp.max(raw, axis=1, keepdims=True), sink)
        raised = jnp.exp(raw - peak)
        total = jnp.sum(raised, axis=1, keepdims=True) + jnp.exp(sink - peak)
        probs = (raised / total).astype(BF).astype(F32)
        newest_prob = (jnp.exp(newest - peak) / total).astype(BF).astype(F32)
        kept = jnp.where(current, 0.0, probs)
        mixed = []
        for u in range(0, group, 2):
            pair = jnp.dot(
                kept[8 * u : 8 * u + 16].astype(BF),
                both(n * group + u),
                preferred_element_type=F32,
            )
            mixed += [pair[:8, :LANES], pair[8:, LANES:]]
        mixed = jnp.concatenate(mixed, axis=0)
        scb[at, :] = mixed + newest_prob * entries
        return c

    lax.fori_loop(0, TOK // group, attend, 0)
    tiles = []
    for tile in range(2):
        even = scb[pl.ds(2 * tile, TOK, stride=8), :]
        odd = scb[pl.ds(2 * tile + 1, TOK, stride=8), :]
        tiles.append(jnp.where(lane < HD, pltpu.roll(even, HD, axis=1), odd).astype(BF))
    attended = jnp.concatenate(tiles, axis=1)

    def out_block(owner):
        return dot_nt(attended, wo[cols(owner), :])

    for n in range(NX):
        mine_b[n] = out_block(2 * n + 1 - core).astype(BF)
    to_sib = pltpu.make_async_remote_copy(
        src_ref=mine_b,
        dst_ref=sib_b,
        send_sem=o_send.at[0],
        recv_sem=o_recv.at[0],
        device_id=(dp, sib),
        device_id_type=MESH,
    )
    to_sib.start()
    for n in range(NX):
        mine_f[n] = out_block(2 * n + core)
    to_sib.wait_recv()

    def to_chip(i):
        owner = lax.rem(xx + i, NX)
        return pltpu.make_async_remote_copy(
            src_ref=chip_b.at[owner],
            dst_ref=recv_b.at[i],
            send_sem=o_send.at[i],
            recv_sem=o_recv.at[i],
            device_id=(dp, owner * 2 + core),
            device_id_type=MESH,
        )

    for i in (2, 1, 3):
        owner = lax.rem(xx + i, NX)
        chip_b[owner] = (mine_f[owner] + sib_b[owner].astype(F32)).astype(BF)
        to_chip(i).start()
    total = tok_pad[...] + (mine_f[xx] + sib_b[xx].astype(F32))
    for get in get_gu:
        get.wait()
    raw_gu[COL:PAD, :] = jnp.zeros((PAD - COL, FULL), BF)
    raw_gu[PAD + COL : 2 * PAD, :] = jnp.zeros((PAD - COL, FULL), BF)
    spread_blocks(raw_gu, wgu, 2 * PAD, 48)
    get_dn.wait()
    raw_dn[COL:PAD, :] = jnp.zeros((PAD - COL, FULL), BF)
    spread_blocks(raw_dn, wdn, PAD, 48)
    for i in (1, 3, 2):
        to_chip(i).wait_recv()
    for i in (1, 2, 3):
        total = total + recv_b[i].astype(F32)
    resid[...] = total

    hid[...] = (total * own_gain[...]).astype(BF)

    def within(i):
        return pl.ds(pl.multiple_of(lax.rem(i, PAIR) * SLOTS, SLOTS), SLOTS)

    def dispatch_copy(j, i):
        dest = lax.rem(z + NZ + NZ - z_offset(j), NZ) * NY + lax.rem(y + NY - i, NY)
        return pltpu.make_async_remote_copy(
            src_ref=placed.at[pl.ds(pl.multiple_of(dest * SLOTS, SLOTS), SLOTS), :],
            dst_ref=rows.at[j * PARTS + lax.div(i, PAIR), within(i), cols(tp)],
            send_sem=d_send.at[j * NY + i],
            recv_sem=d_recv.at[j * NY + i],
            device_id=(dest, tp),
            device_id_type=MESH,
        )

    own_in = pltpu.make_async_copy(
        placed.at[pl.ds(pl.multiple_of(dp * SLOTS, SLOTS), SLOTS), :],
        rows.at[OWN * PARTS, pl.ds(0, SLOTS), cols(tp)],
        lsem.at[0],
    )

    def dispatch(j, c):
        zd = lax.rem(z + NZ + NZ - z_offset(j), NZ)
        part = pl.ds(pl.multiple_of(zd * GROUP, GROUP), GROUP)
        placed[part, :] = jnp.dot(
            placer[part, :].astype(BF), hid[...], preferred_element_type=F32
        ).astype(BF)

        @pl.when(j == OWN)
        def _():
            own_in.start()

        @pl.when(j != OWN)
        def _():
            dispatch_copy(j, 0).start()

        for i in range(1, NY):
            dispatch_copy(j, i).start()
        return c

    lax.fori_loop(0, AHEAD, dispatch, 0)

    lifted = total * own_gain[...]
    wide_rows = jnp.zeros((LANES - TOK, PAD), BF)
    logit_part = jnp.zeros((experts, LANES), F32)
    for piece in split3(lifted):
        logit_part = logit_part + dot_nt(router_pad[...], jnp.concatenate([piece, wide_rows], axis=0))
    square_part = jnp.zeros((8, LANES), F32)
    ones = jnp.ones((8, PAD), BF)
    for piece in split3(total * total):
        square_part = square_part + dot_nt(ones, jnp.concatenate([piece, wide_rows], axis=0))
    small_t[tp, 0:experts, :] = logit_part
    small_t[tp, experts : experts + 8, :] = square_part

    def share(i):
        return pltpu.make_async_remote_copy(
            src_ref=small_t.at[tp],
            dst_ref=small_t.at[tp],
            send_sem=a_send.at[i],
            recv_sem=a_recv.at[i],
            device_id=(dp, lax.rem(tp + i, NTP)),
            device_id_type=MESH,
        )

    for i in range(1, NTP):
        share(i).start()

    def scale_copy(j, i):
        zd = lax.rem(z + NZ - z_offset(j), NZ)
        dest = zd * NY + lax.rem(y + NY - i, NY)
        return pltpu.make_async_remote_copy(
            src_ref=scale_out.at[zd],
            dst_ref=scale_in.at[j * NY + i],
            send_sem=s_send.at[j * NY + i],
            recv_sem=s_recv.at[j * NY + i],
            device_id=(dest, tp),
            device_id_type=MESH,
        )

    def scales_of(c):
        spot = lax.broadcasted_iota(jnp.int32, (1, LANES), 1)
        line = jnp.zeros((1, LANES), F32)
        for k in range(PAIR):
            n = c * PAIR + k

            @pl.when(n != OWN * NY)
            def _():
                scale_copy(lax.div(n, NY), lax.rem(n, NY)).wait_recv()

            there = pltpu.roll(
                jnp.broadcast_to(scale_in[n], (8, LANES)),
                lax.rem(k + NY - y, NY) * SLOTS,
                axis=1,
            )[0:1]
            line = jnp.where(lax.div(spot, SLOTS) == k, there, line)
        return jnp.transpose(jnp.broadcast_to(line, (LANES, LANES)))[:CHUNK, :1]

    def sums():
        summed = small_t[0]
        for n in range(1, NTP):
            summed = summed + small_t[n]
        scale_row = lax.rsqrt(summed[experts : experts + 1, :] * (1.0 / FULL) + norm_eps)
        return summed, scale_row

    def settle():
        for i in range(1, NTP):
            share(i).wait_recv()
        scale_row = sums()[1]
        hi, mid, low = split3(jnp.broadcast_to(scale_row[:, :TOK], (8, TOK)))
        which = lax.broadcasted_iota(jnp.int32, (8, TOK), 0)
        stacked = jnp.where(
            which == 0,
            hi.astype(F32),
            jnp.where(which == 1, mid.astype(F32), jnp.where(which == 2, low.astype(F32), 0.0)),
        ).astype(BF)
        for n in range(NZ):
            at = slice(n * GROUP, (n + 1) * GROUP)
            spots = placer[at, :].astype(BF)
            scale_out[n] = jnp.sum(dot_nt(stacked, spots), axis=0, keepdims=True)
        scale_in[OWN * NY] = scale_out[z]

        def send_scale(n, c):
            j, i = lax.div(n, NY), lax.rem(n, NY)

            @pl.when(n != OWN * NY)
            def _():
                scale_copy(j, i).start()

            return c

        lax.fori_loop(0, NZ * NY, send_scale, 0)

    def combine_weights():
        summed, scale_row = sums()
        logits = summed[0:experts, :TOK] * scale_row[:, :TOK]
        lifted_logits = jnp.where(named, jnp.exp(logits), 0.0)
        weights = lifted_logits / jnp.sum(lifted_logits, axis=0, keepdims=True)
        for e in range(experts):
            at = slice(e * SLOTS, (e + 1) * SLOTS)
            placer[at, :] = placer[at, :] * weights[e : e + 1, :]
        for n in range(NZ):
            at = slice(n * GROUP, (n + 1) * GROUP)
            piece = jnp.transpose(placer[at, :])
            hi = piece.astype(BF)
            comb_hi[:, at] = hi
            comb_lo[:, at] = (piece - hi.astype(F32)).astype(BF)

    def back_copy(j, i):
        home = lax.rem(z + z_offset(j), NZ) * NY + lax.rem(y + i, NY)
        return pltpu.make_async_remote_copy(
            src_ref=made.at[j * PARTS + lax.div(i, PAIR), within(i), :],
            dst_ref=back.at[pl.ds(pl.multiple_of(dp * SLOTS, SLOTS), SLOTS), :],
            send_sem=r_send.at[j * NY + i],
            recv_sem=r_recv.at[dp],
            device_id=(home, tp),
            device_id_type=MESH,
        )

    own_back = pltpu.make_async_copy(
        made.at[OWN * PARTS, pl.ds(0, SLOTS), :],
        back.at[pl.ds(pl.multiple_of(dp * SLOTS, SLOTS), SLOTS), :],
        lsem.at[1],
    )

    def step(t, c):
        @pl.when(t < NC)
        def _():
            for k in range(PAIR):
                n = t * PAIR + k

                @pl.when(n == OWN * NY)
                def _():
                    own_in.wait()

                @pl.when(n != OWN * NY)
                def _():
                    dispatch_copy(lax.div(n, NY), lax.rem(n, NY)).wait_recv()

            send_own(rows, 0, t)

        @pl.when(t == SETTLE)
        def _():
            settle()

        @pl.when((t >= ON) & (t < NC + ON))
        def _():
            send_on(rows, 0, t - ON)

        @pl.when((lax.rem(t, PARTS) == 0) & (t < (NZ - AHEAD) * PARTS))
        def _():
            dispatch(lax.div(t, PARTS) + AHEAD, 0)

        @pl.when((t >= GATE) & (t < NC + GATE))
        def _():
            j = t - GATE
            scales = scales_of(j)
            all_in(rows, 0, j)
            mixed = dot_nt(rows[j], wgu[...]) * scales
            gate = mixed[:, :PAD]
            up = mixed[:, PAD:]
            act = gate * jax.nn.sigmoid(glu_alpha * gate) * (up + 1.0)
            acts[j, :, cols(tp)] = act.astype(BF)
            send_own(acts, 1, j)

        @pl.when((t >= FAR) & (t < NC + FAR))
        def _():
            send_far(rows, 0, t - FAR)

        @pl.when((t >= ACT_ON) & (t < NC + ACT_ON))
        def _():
            send_on(acts, 1, t - ACT_ON)

        @pl.when(t == (NZ - AHEAD) * PARTS + 1)
        def _():
            combine_weights()

        @pl.when((t >= DOWN) & (t < NC + DOWN))
        def _():
            j = t - DOWN
            all_in(acts, 1, j)
            made[j] = dot_nt(acts[j], wdn[...]).astype(BF)
            for k in range(PAIR):
                n = j * PAIR + k

                @pl.when(n == OWN * NY)
                def _():
                    own_back.start()

                @pl.when(n != OWN * NY)
                def _():
                    back_copy(lax.div(n, NY), lax.rem(n, NY)).start()

        @pl.when((t >= ACT_FAR) & (t < NC + ACT_FAR))
        def _():
            send_far(acts, 1, t - ACT_FAR)

        return c

    lax.fori_loop(0, NC + DOWN, step, 0)

    to_sib.wait_send()
    for i in range(1, NX):
        to_chip(i).wait_send()
    for i in range(1, NTP):
        share(i).wait_send()
    all_sent(toks, 2, 0)

    def sent(n, c):
        @pl.when(n != OWN * NY)
        def _():
            j, i = lax.div(n, NY), lax.rem(n, NY)
            dispatch_copy(j, i).wait_send()
            back_copy(j, i).wait_send()
            scale_copy(j, i).wait_send()

        return c

    lax.fori_loop(0, NZ * NY, sent, 0)

    def sent_x(j, c):
        all_sent(rows, 0, j)
        all_sent(acts, 1, j)
        return c

    lax.fori_loop(0, NC, sent_x, 0)

    def await_back(i, c):
        peer = lax.rem(dp + i, NZ * NY)
        pltpu.make_async_remote_copy(
            src_ref=made.at[0, pl.ds(0, SLOTS), :],
            dst_ref=back.at[pl.ds(pl.multiple_of(peer * SLOTS, SLOTS), SLOTS), :],
            send_sem=r_send.at[1],
            recv_sem=r_recv.at[peer],
            device_id=(peer, tp),
            device_id_type=MESH,
        ).wait_recv()
        return c

    own_back.wait()
    lax.fori_loop(1, NZ * NY, await_back, 0)
    got = back[...]
    answer = (
        resid[...]
        + jnp.dot(comb_hi[...], got, preferred_element_type=F32)
        + jnp.dot(comb_lo[...], got, preferred_element_type=F32)
    )
    out[...] = answer[:, :COL]


def on_device(
    tokens,
    attn_gain,
    w_query,
    w_keyvalue,
    attn_sinks,
    w_out,
    window_cache,
    positions,
    moe_gain,
    router,
    gate_up,
    w_down,
    expert_ids,
):
    vmem = pl.BlockSpec(memory_space=pltpu.VMEM)
    hbm = pl.BlockSpec(memory_space=pl.ANY)
    dma = pltpu.SemaphoreType.DMA
    vm = pltpu.VMEM
    return pl.pallas_call(
        layer_body,
        out_shape=jax.ShapeDtypeStruct(tokens.shape, F32),
        in_specs=[hbm] * 13,
        out_specs=vmem,
        scratch_shapes=[
            vm((NC, CHUNK, WIDE), BF),
            vm((NC, CHUNK, WIDE), BF),
            vm((2 * PAD, WIDE), BF),
            vm((PAD, WIDE), BF),
            vm((NZ * GROUP, PAD), BF),
            vm((NC, CHUNK, PAD), BF),
            vm((NZ * GROUP, PAD), BF),
            vm((1, TOK, WIDE), BF),
            vm((WIDE, HEADS * HD), BF),
            vm((WIDE, 2 * HD), BF),
            vm((WIDE, HEADS * HD), BF),
            vm((TOK, LANES, 2 * HD), BF),
            vm((2 * PAD, FULL), BF),
            vm((PAD, FULL), BF),
            vm((TOK, COL), BF),
            vm((FULL,), F32),
            vm((FULL,), F32),
            pltpu.SMEM((HEADS,), F32),
            vm((1, TOK), jnp.int32),
            vm((NZ * NY, COL), BF),
            vm((expert_ids.shape[1], TOK), jnp.int32),
            vm((1, WIDE), F32),
            vm((1, PAD), F32),
            vm((TOK, PAD), F32),
            vm((SPAN, LANES), F32),
            vm((SPAN, LANES), F32),
            vm((SPAN, LANES), F32),
            vm((TOK, PAD), F32),
            vm((TOK, PAD), BF),
            vm((NZ * GROUP, TOK), F32),
            vm((TOK, NZ * GROUP), BF),
            vm((TOK, NZ * GROUP), BF),
            vm((NX, TOK, PAD), F32),
            vm((NX, TOK, PAD), BF),
            vm((NX, TOK, PAD), BF),
            vm((NX, TOK, PAD), BF),
            vm((NX, TOK, PAD), BF),
            vm((2, TOK, LANES), F32),
            vm((8, LANES), F32),
            vm((NTP, 40, LANES), F32),
            vm((SPAN, LANES), F32),
            vm((NZ * NY, PAD), BF),
            vm((NZ, 1, LANES), F32),
            vm((NZ * NY, 1, LANES), F32),
            dma((35,)),
            dma((2,)),
            dma((NZ * NY,)),
            dma((NZ * NY,)),
            dma((NZ * NY,)),
            dma((NZ * NY,)),
            dma((3, 8, NC)),
            dma((3, 8, NC)),
            dma((NX,)),
            dma((NX,)),
            dma((NTP,)),
            dma((NTP,)),
            dma((NZ * NY,)),
            dma((NZ * NY,)),
        ],
        compiler_params=pltpu.CompilerParams(
            collective_id=0, has_side_effects=True, vmem_limit_bytes=60 * 1024 * 1024
        ),
        name="layer",
    )(
        tokens,
        attn_gain,
        moe_gain,
        attn_sinks,
        positions[None, :],
        jnp.transpose(router),
        jnp.transpose(expert_ids),
        w_query,
        w_keyvalue.reshape(FULL, 2 * HD),
        jnp.transpose(w_out),
        window_cache.reshape(TOK, LANES, 2 * HD),
        jnp.transpose(gate_up[0], (1, 2, 0)),
        jnp.transpose(w_down[0]),
    )


def solution(mesh):
    in_specs = (
        P("dp", "tp"),
        P(),
        P(None, "tp"),
        P(None, "tp", None),
        P("tp"),
        P("tp", None),
        P("dp", "tp", None, None),
        P("dp"),
        P(),
        P("tp", None),
        P("dp", None, None, "tp"),
        P("dp", None, "tp"),
        P("dp", None),
    )
    out_specs = P("dp", "tp")
    return jax.shard_map(
        on_device, mesh=mesh, in_specs=in_specs, out_specs=out_specs, check_vma=False
    )
```
